128 devices in a mesh: front: 4 (over z), grid: 32 (over x, y, core).
Axes of the slice: x: 4, y: 4, z: 4, core: 2. Of those that a mesh axis runs over, the one named last changes fastest.
Arguments:
- child_fronts: float32 [4, 6144, 6144], P('front', 'grid'), as said below
- parent_fronts: float32 [4, 6144, 6144], P('front', 'grid'), as said below
- child_maps: int32 [4, 6144], replicated, may hold values from 0 to 6143, as said below
- parent_of: int32 [4], replicated, may hold values from 0 to 3
- child_pivots: int32 [4], replicated, may hold values from 64 to 256, as said below
- parent_pivots: int32 [4], replicated, may hold values from 64 to 256, as said below
Outputs:
- child_panels: float32 [4, 6144, 256], P('front', 'grid')
- parent_panels: float32 [4, 6144, 256], P('front', 'grid')
- parent_schur: float32 [4, 6144, 6144], P('front', 'grid')
The draws below stay inside these ranges and needn't reach their ends.
Inputs may be any that keep to these rules, and one draw needn't show every extreme that they name: Each row of child_maps is a permutation: row i of lower front c becomes row child_maps[c, i] of its parent. For i from child_pivots[c] on, child_maps[c, i] strictly increases with i; the rows below child_pivots[c] take the remaining parent indices in increasing order. `parent_of`: entry c names the upper front that receives the contribution block of lower front c. Lower front c eliminates its first child_pivots[c] variables; in every draw some front has exactly 256. Upper front q eliminates its first parent_pivots[q] variables; in every draw some front has exactly 256. `child_fronts`: every front is symmetric positive definite. `parent_fronts`: every front is symmetric positive definite.
All inputs are finite; a program needn't handle non-finite values.
Results may differ from the reference program's by a relative error of at most 0.00011.
Values sent between devices are 32-bit elements; how exact they have to be, the bound alone decides.
A program may use at most 128 MiB of HBM per device.

```python
import jax
import jax.numpy as jnp
from jax import lax

F = 6144
PMAX = 256
FRONTS = 4


def coupled_fronts(key):

    def one_front(front_index):
        subkey = jax.random.fold_in(key, front_index)
        factor_matrix = jax.random.normal(jax.random.fold_in(subkey, 1), (F, F), jnp.float32)
        diagonal = jax.random.uniform(jax.random.fold_in(subkey, 2), (F,), jnp.float32, 0.5, 1.0)
        gram = jnp.dot(factor_matrix, factor_matrix.T, precision=lax.Precision.HIGHEST, preferred_element_type=jnp.float32) / F
        return (gram + gram.T) * 0.5 + jnp.diag(diagonal)
    return lax.map(one_front, jnp.arange(FRONTS, dtype=jnp.int32))


def draw_child_fronts(key, part):
    return coupled_fronts(jax.random.fold_in(key, 21))


def draw_parent_fronts(key, part):
    return coupled_fronts(jax.random.fold_in(key, 22))


def pivot_counts(key):
    counts = jax.random.randint(jax.random.fold_in(key, 3), (FRONTS,), PMAX // 4, PMAX + 1)
    chosen = jax.random.randint(jax.random.fold_in(key, 4), (), 0, FRONTS)
    return counts.at[chosen].set(PMAX).astype(jnp.int32)


def increasing_maps(key, pivots):

    def one_front(front_index, pivot_count):
        shuffled = jax.random.permutation(jax.random.fold_in(key, front_index), F).astype(jnp.int32)
        position_of = jnp.argsort(shuffled).astype(jnp.int32)
        chosen = (position_of < F - pivot_count).astype(jnp.int32)
        scores = chosen * F + jnp.arange(F, dtype=jnp.int32)
        return jnp.argsort(scores).astype(jnp.int32)
    return jax.vmap(one_front)(jnp.arange(FRONTS, dtype=jnp.int32), pivots)


def draw_child_pivots(key, part):
    return pivot_counts(jax.random.fold_in(key, 11))


def draw_parent_pivots(key, part):
    return pivot_counts(jax.random.fold_in(key, 12))


def draw_child_maps(key, part):
    pivots = pivot_counts(jax.random.fold_in(key, 11))
    return increasing_maps(jax.random.fold_in(key, 13), pivots)


def touch_ends(entries, key, low, top_value):
    shape = entries.shape
    place = [jax.random.randint(jax.random.fold_in(key, axis), (), 0, shape[axis]) for axis in range(len(shape))]
    entries = entries.at[tuple(place)].set(low)
    longest = shape.index(max(shape))
    place[longest] = (place[longest] + 1) % shape[longest]
    return entries.at[tuple(place)].set(top_value)


def setup_inputs(seed: int = 0) -> dict:
    keys = jax.random.split(jax.random.key(seed), 7)
    return {
        "child_fronts": draw_child_fronts(jax.random.fold_in(keys[6], 71), 0),
        "parent_fronts": draw_parent_fronts(jax.random.fold_in(keys[6], 71), 0),
        "child_maps": draw_child_maps(jax.random.fold_in(keys[6], 71), 0),
        "parent_of": touch_ends(jax.random.randint(keys[3], (FRONTS,), 0, FRONTS), jax.random.fold_in(keys[3], 1), 0, FRONTS - 1).astype(jnp.int32),
        "child_pivots": draw_child_pivots(jax.random.fold_in(keys[6], 71), 0),
        "parent_pivots": draw_parent_pivots(jax.random.fold_in(keys[6], 71), 0),
    }


def partial_factor(front_matrix, pivots):
    position = jnp.arange(PMAX, dtype=jnp.int32)
    pivot_mask = (position < pivots).astype(jnp.float32)
    pivot_block = front_matrix[:PMAX, :PMAX] * pivot_mask[:, None] * pivot_mask[None, :] + jnp.diag(1.0 - pivot_mask)
    factor_low = jnp.linalg.cholesky(pivot_block)
    columns = front_matrix[:, :PMAX] * pivot_mask[None, :]
    panel_rows = jax.scipy.linalg.solve_triangular(factor_low, columns.T, lower=True).T
    product = jnp.dot(panel_rows.astype(jnp.float32), panel_rows.T.astype(jnp.float32), precision=lax.Precision.HIGHEST, preferred_element_type=jnp.float32)
    every = jnp.arange(F, dtype=jnp.int32)
    remain_mask = (every >= pivots).astype(jnp.float32)
    schur_rows = (front_matrix - product) * remain_mask[:, None] * remain_mask[None, :]
    return (panel_rows, schur_rows)

def reference(child_fronts, parent_fronts, child_maps, parent_of, child_pivots, parent_pivots):
    child_list = []
    totals = [parent_fronts[parent_index] for parent_index in range(FRONTS)]
    for child_index in range(FRONTS):
        panel_rows, schur_rows = partial_factor(child_fronts[child_index], child_pivots[child_index])
        child_list.append(panel_rows)
        inverse = jnp.argsort(child_maps[child_index]).astype(jnp.int32)
        moved = jnp.take(jnp.take(schur_rows, inverse, axis=0), inverse, axis=1)
        for parent_index in range(FRONTS):
            weight = (parent_of[child_index] == parent_index).astype(jnp.float32)
            totals[parent_index] = totals[parent_index] + weight * moved
    parent_list = []
    schur_list = []
    for parent_index in range(FRONTS):
        panel_rows, schur_rows = partial_factor(totals[parent_index], parent_pivots[parent_index])
        parent_list.append(panel_rows)
        schur_list.append(schur_rows)
    return (jnp.stack(child_list), jnp.stack(parent_list), jnp.stack(schur_list))
```

```python
import functools

import jax
import jax.numpy as jnp
from jax import lax
from jax.experimental import pallas as pl
from jax.experimental.pallas import tpu as pltpu
from jax.sharding import PartitionSpec as P

PMAX = 256
CHIPS = 16
SIDE = 4
ROWS = 192
WIDE = 384
ORDER = 6144
BASE = 32
F32 = jnp.float32
BF16 = jnp.bfloat16
VMEM = pltpu.VMEM
NT = (((1,), (1,)), ((), ()))
NN = (((1,), (0,)), ((), ()))
TN = (((0,), (0,)), ((), ()))


def dot(a, b, dims):
    return lax.dot_general(a, b, dims, preferred_element_type=F32)


def split(a):
    high = a.astype(BF16)
    low = (a - high.astype(F32)).astype(BF16)
    return high, low


def product(a, b, dims):
    a_high, a_low = split(a)
    b_high, b_low = split(b)
    return dot(a_high, b_high, dims) + (dot(a_high, b_low, dims) + dot(a_low, b_high, dims))


def pick(one_hot, a, dims):
    a_high, a_low = split(a)
    return dot(one_hot, a_high, dims) + dot(one_hot, a_low, dims)


def cholesky_kernel(block_ref, inverse_ref, work):
    rows = lax.broadcasted_iota(jnp.int32, (PMAX, PMAX), 0)
    columns = lax.broadcasted_iota(jnp.int32, (PMAX, PMAX), 1)
    work[:, :PMAX] = block_ref[...]
    work[:, PMAX:] = (rows == columns).astype(F32)
    small_rows = lax.broadcasted_iota(jnp.int32, (BASE, 1), 0)
    eye_rows = lax.broadcasted_iota(jnp.int32, (BASE, BASE), 0)
    eye_columns = lax.broadcasted_iota(jnp.int32, (BASE, BASE), 1)
    eye = (eye_rows == eye_columns).astype(F32)
    for step in range(PMAX // BASE):
        first = step * BASE
        last = first + BASE
        diagonal = work[first:last, first:last]
        both = jnp.concatenate([diagonal, eye, jnp.zeros((BASE, 128 - 2 * BASE), F32)], axis=1)
        for k in range(BASE - 1):
            column = both[:, k : k + 1]
            row = both[k : k + 1, :]
            factor = jnp.where(small_rows > k, column / row[:, k : k + 1], 0.0)
            both = both - factor * row
        pivots = jnp.sum(both[:, :BASE] * eye, axis=1, keepdims=True)
        inverse = both[:, BASE : 2 * BASE] / jnp.sqrt(pivots)
        strip = lax.dot_general(
            inverse, work[first:last, :], NN, precision=lax.Precision.HIGHEST, preferred_element_type=F32
        )
        work[first:last, :] = strip
        if last < PMAX:
            update = lax.dot_general(
                strip[:, :PMAX], strip, TN, precision=lax.Precision.HIGHEST, preferred_element_type=F32
            )
            work[last:, :] = work[last:, :] - update[last:, :]
    inverse_ref[...] = work[:, PMAX:]


def inverse_factor(pivot_block):
    return pl.pallas_call(
        cholesky_kernel,
        out_shape=jax.ShapeDtypeStruct((PMAX, PMAX), F32),
        in_specs=[pl.BlockSpec(memory_space=VMEM)],
        out_specs=pl.BlockSpec(memory_space=VMEM),
        scratch_shapes=[pltpu.VMEM((PMAX, 2 * PMAX), F32)],
        cost_estimate=pl.CostEstimate(flops=200_000_000, bytes_accessed=524288, transcendentals=0),
        name="inverse_factor",
    )(pivot_block)


def turn_kernel(map_here, map_next, even_here, even_next, odd_here, odd_next, out_ref, window, places):
    core = lax.axis_index("grid") % 2
    block = pl.program_id(0)
    window[:ROWS, :WIDE] = even_here[...]
    window[:ROWS, WIDE:] = even_next[...]
    window[ROWS:, :WIDE] = odd_here[...]
    window[ROWS:, WIDE:] = odd_next[...]
    places[:, :WIDE] = map_here[...]
    places[:, WIDE:] = map_next[...]
    lanes = pl.ds(pl.multiple_of(core * 128, 128), 512)
    first = block * WIDE + core * ROWS
    wanted = first + lax.broadcasted_iota(jnp.int32, (ROWS, 512), 0)
    one_hot = (wanted == places[:1, lanes]).astype(F32).astype(BF16)
    out_ref[0] = pick(one_hot, window[:, lanes], NT)


def turn(even, odd, places):
    here = lambda rows: pl.BlockSpec((rows, WIDE), lambda j: (0, j))
    after = lambda rows: pl.BlockSpec((rows, WIDE), lambda j: (0, jnp.minimum(j + 1, CHIPS - 1)))
    after_map = pl.BlockSpec((8, WIDE), lambda j: (0, j + 1))
    return pl.pallas_call(
        turn_kernel,
        grid=(CHIPS,),
        out_shape=jax.ShapeDtypeStruct((CHIPS, ROWS, WIDE), F32),
        in_specs=[here(8), after_map, here(ROWS), after(ROWS), here(ROWS), after(ROWS)],
        out_specs=pl.BlockSpec((1, ROWS, WIDE), lambda j: (j, 0, 0)),
        scratch_shapes=[pltpu.VMEM((WIDE, 2 * WIDE), F32), pltpu.VMEM((8, 2 * WIDE), jnp.int32)],
        cost_estimate=pl.CostEstimate(flops=4_000_000_000, bytes_accessed=15_000_000, transcendentals=0),
        name="turn",
    )(places, places, even, even, odd, odd)


def child_kernel(
    map_own, map_before, map_here, own_ref, window_ref, all_ref, inverse_ref, moved_ref,
    panel_ref, schur_ref, strip, places, panel_rows,
):
    step = pl.program_id(0)
    grid_rank = lax.axis_index("grid")
    inverse = inverse_ref[...]

    @pl.when(step == 0)
    def _():
        panel_ref[...] = product(own_ref[...], inverse, NT)
        wanted = grid_rank * ROWS + lax.broadcasted_iota(jnp.int32, (ROWS, 512), 0)
        one_hot = (wanted == map_own[:1, :]).astype(F32).astype(BF16)
        panel_rows[...] = product(pick(one_hot, window_ref[...], NN), inverse, NT)

    strip[:, :WIDE] = strip[:, WIDE:]

    @pl.when(step < CHIPS)
    def _():
        panel = product(all_ref[...], inverse, NT)
        strip[:, WIDE:] = moved_ref[0] - product(panel_rows[...], panel, NT)

    @pl.when(step == CHIPS)
    def _():
        strip[:, WIDE:] = jnp.zeros((ROWS, WIDE), F32)

    @pl.when(step > 0)
    def _():
        places[:, :WIDE] = map_before[...]
        places[:, WIDE:] = map_here[...]
        wanted = (step - 1) * WIDE + lax.broadcasted_iota(jnp.int32, (WIDE, 640), 0)
        one_hot = (wanted == places[:1, :640]).astype(F32).astype(BF16)
        high, low = split(strip[:, :640])
        schur_ref[0] = dot(high, one_hot, NT) + dot(low, one_hot, NT)


def child_schur(places, own_places, own, window, columns, inverse, moved):
    last = CHIPS - 1
    return pl.pallas_call(
        child_kernel,
        grid=(CHIPS + 1,),
        out_shape=(
            jax.ShapeDtypeStruct((ROWS, PMAX), F32),
            jax.ShapeDtypeStruct((CHIPS, ROWS, WIDE), F32),
        ),
        in_specs=[
            pl.BlockSpec((8, 512), lambda j: (0, 0)),
            pl.BlockSpec((8, WIDE), lambda j: (0, jnp.maximum(j - 1, 0))),
            pl.BlockSpec((8, WIDE), lambda j: (0, j)),
            pl.BlockSpec((ROWS, PMAX), lambda j: (0, 0)),
            pl.BlockSpec((512, PMAX), lambda j: (0, 0)),
            pl.BlockSpec((WIDE, PMAX), lambda j: (jnp.minimum(j, last), 0)),
            pl.BlockSpec((PMAX, PMAX), lambda j: (0, 0)),
            pl.BlockSpec((1, ROWS, WIDE), lambda j: (jnp.minimum(j, last), 0, 0)),
        ],
        out_specs=(
            pl.BlockSpec((ROWS, PMAX), lambda j: (0, 0)),
            pl.BlockSpec((1, ROWS, WIDE), lambda j: (jnp.maximum(j - 1, 0), 0, 0)),
        ),
        scratch_shapes=[
            pltpu.VMEM((ROWS, 2 * WIDE), F32),
            pltpu.VMEM((8, 2 * WIDE), jnp.int32),
            pltpu.VMEM((ROWS, PMAX), F32),
        ],
        cost_estimate=pl.CostEstimate(flops=8_000_000_000, bytes_accessed=20_000_000, transcendentals=0),
        name="child_schur",
    )(own_places, places, places, own, window, columns, inverse, moved)


def parent_kernel(
    pivots_ref, weight_ref, own_ref, all_ref, inverse_ref, children_ref, front_ref, panel_ref, schur_ref, panel_rows
):
    step = pl.program_id(0)
    grid_rank = lax.axis_index("grid")
    inverse = inverse_ref[...]

    @pl.when(step == 0)
    def _():
        panel_rows[...] = product(own_ref[...], inverse, NT)
        panel_ref[...] = panel_rows[...]

    panel = product(all_ref[...], inverse, NT)
    total = front_ref[...] - product(panel_rows[...], panel, NT)
    for child in range(SIDE):
        total = total + weight_ref[child] * children_ref[child, 0]
    pivots = pivots_ref[0]
    rows = grid_rank * ROWS + lax.broadcasted_iota(jnp.int32, (ROWS, WIDE), 0)
    columns = step * WIDE + lax.broadcasted_iota(jnp.int32, (ROWS, WIDE), 1)
    schur_ref[...] = jnp.where((rows >= pivots) & (columns >= pivots), total, 0.0)


def parent_schur(pivots, weights, own, columns, inverse, children, front):
    smem = pl.BlockSpec(memory_space=pltpu.SMEM)
    return pl.pallas_call(
        parent_kernel,
        grid=(CHIPS,),
        out_shape=(jax.ShapeDtypeStruct((ROWS, PMAX), F32), jax.ShapeDtypeStruct((ROWS, ORDER), F32)),
        in_specs=[
            smem,
            smem,
            pl.BlockSpec((ROWS, PMAX), lambda j: (0, 0)),
            pl.BlockSpec((WIDE, PMAX), lambda j: (j, 0)),
            pl.BlockSpec((PMAX, PMAX), lambda j: (0, 0)),
            pl.BlockSpec((SIDE, 1, ROWS, WIDE), lambda j: (0, j, 0, 0)),
            pl.BlockSpec((ROWS, WIDE), lambda j: (0, j)),
        ],
        out_specs=(
            pl.BlockSpec((ROWS, PMAX), lambda j: (0, 0)),
            pl.BlockSpec((ROWS, WIDE), lambda j: (0, j)),
        ),
        scratch_shapes=[pltpu.VMEM((ROWS, PMAX), F32)],
        cost_estimate=pl.CostEstimate(flops=4_000_000_000, bytes_accessed=35_000_000, transcendentals=0),
        name="parent_schur",
    )(pivots, weights, own, columns, inverse, children, front)


def pivot_mask(pivots):
    return (jnp.arange(PMAX, dtype=jnp.int32) < pivots).astype(F32)


def pivot_block(columns, mask):
    return columns[:PMAX] * mask[:, None] + jnp.diag(1.0 - mask)


def on_device(child_fronts, parent_fronts, child_maps, parent_of, child_pivots, parent_pivots):
    front_group = lax.axis_index("front")
    grid_rank = lax.axis_index("grid")
    core = grid_rank % 2
    front_rows = child_fronts[0]
    child_map = child_maps[front_group]
    pivots = child_pivots[front_group]

    sibling = lax.ppermute(front_rows, "grid", [(g, g ^ 1) for g in range(2 * CHIPS)])
    even = jnp.where(core == 0, front_rows, sibling)
    odd = jnp.where(core == 0, sibling, front_rows)
    position = jnp.arange(ORDER, dtype=jnp.int32)
    line = jnp.where(position >= pivots, child_map, -1)
    line = jnp.pad(line, (0, 2 * WIDE), constant_values=-1)
    places = jnp.broadcast_to(line[None], (8, line.shape[0]))
    turned = turn(even, odd, places)
    same_core = [[2 * chip + k for chip in range(CHIPS)] for k in range(2)]
    moved = lax.all_to_all(turned, "grid", 0, 0, axis_index_groups=same_core)

    mask = pivot_mask(pivots)
    own = front_rows[:, :PMAX] * mask[None, :]
    columns = lax.all_gather(own, "grid", axis=0, tiled=True)
    inverse = inverse_factor(pivot_block(columns, mask))
    first = grid_rank * ROWS
    start = jnp.minimum(first, ORDER - 512)
    window = lax.dynamic_slice(columns, (start, 0), (512, PMAX))
    own_places = lax.dynamic_slice(places, (0, start), (8, 512))
    panel_rows, schur = child_schur(places, own_places, own, window, columns, inverse, moved)

    upper_pivots = parent_pivots[front_group]
    upper_mask = pivot_mask(upper_pivots)
    weights = (parent_of == front_group).astype(F32)
    leading = lax.all_gather(schur[0, :, :PMAX], "front", axis=0)
    upper_own = parent_fronts[0, :, :PMAX]
    for child in range(SIDE):
        upper_own = upper_own + weights[child] * leading[child]
    upper_own = upper_own * upper_mask[None, :]
    upper_columns = lax.all_gather(upper_own, "grid", axis=0, tiled=True)
    children = lax.all_gather(schur, "front", axis=0)
    upper_inverse = inverse_factor(pivot_block(upper_columns, upper_mask))
    upper_panel, upper_schur = parent_schur(
        upper_pivots[None], weights, upper_own, upper_columns, upper_inverse, children, parent_fronts[0]
    )
    return (panel_rows[None], upper_panel[None], upper_schur[None])


def solution(mesh):
    in_specs = (P("front", "grid", None), P("front", "grid", None), P(), P(), P(), P())
    out_specs = (P("front", "grid", None), P("front", "grid", None), P("front", "grid", None))
    return jax.shard_map(
        on_device, mesh=mesh, in_specs=in_specs, out_specs=out_specs, check_vma=False
    )
```

```python
import functools

import jax
import jax.numpy as jnp
from jax import lax
from jax.experimental import pallas as pl
from jax.experimental.pallas import tpu as pltpu
from jax.sharding import PartitionSpec as P

PMAX = 256
CHIPS = 16
SIDE = 4
ROWS = 192
WIDE = 384
ORDER = 6144
BASE = 32
LEAD = 256
MESH = pl.DeviceIdType.MESH
SELF = ((0, 0), (0, 2), (2, 0), (2, 2))
TURNED = ((0, 1), (1, 0), (3, 3), (3, 1), (1, 2), (2, 3))
F32 = jnp.float32
BF16 = jnp.bfloat16
VMEM = pltpu.VMEM
NT = (((1,), (1,)), ((), ()))
NN = (((1,), (0,)), ((), ()))
TN = (((0,), (0,)), ((), ()))


def dot(a, b, dims):
    return lax.dot_general(a, b, dims, preferred_element_type=F32)


def split(a):
    high = a.astype(BF16)
    low = (a - high.astype(F32)).astype(BF16)
    return high, low


def product(a, b, dims):
    a_high, a_low = split(a)
    b_high, b_low = split(b)
    return dot(a_high, b_high, dims) + (dot(a_high, b_low, dims) + dot(a_low, b_high, dims))


def pick(one_hot, a, dims):
    a_high, a_low = split(a)
    return dot(one_hot, a_high, dims) + dot(one_hot, a_low, dims)


def exact(a, b, dims):
    return lax.dot_general(a, b, dims, precision=lax.Precision.HIGHEST, preferred_element_type=F32)


def shifted(chip, offset, sign=1):
    x = (chip // SIDE + sign * offset[0] + SIDE) % SIDE
    y = (chip % SIDE + sign * offset[1] + SIDE) % SIDE
    return x * SIDE + y


def remote(src, dst, sems, index, device):
    return pltpu.make_async_remote_copy(
        src_ref=src, dst_ref=dst, send_sem=sems[0].at[index], recv_sem=sems[1].at[index],
        device_id=device, device_id_type=MESH,
    )


def greet(devices):
    barrier = pltpu.get_barrier_semaphore()
    for device in devices:
        pl.semaphore_signal(barrier, inc=1, device_id=device, device_id_type=MESH)
    pl.semaphore_wait(barrier, len(devices))


def cholesky_kernel(pivots_ref, block_ref, inverse_ref, work):
    rows = lax.broadcasted_iota(jnp.int32, (PMAX, PMAX), 0)
    columns = lax.broadcasted_iota(jnp.int32, (PMAX, PMAX), 1)
    same = (rows == columns).astype(F32)
    pivots = pivots_ref[0]
    work[:, :PMAX] = jnp.where((rows < pivots) & (columns < pivots), block_ref[...], same)
    work[:, PMAX:] = same
    small_rows = lax.broadcasted_iota(jnp.int32, (BASE, 1), 0)
    eye_rows = lax.broadcasted_iota(jnp.int32, (BASE, BASE), 0)
    eye_columns = lax.broadcasted_iota(jnp.int32, (BASE, BASE), 1)
    eye = (eye_rows == eye_columns).astype(F32)
    for step in range(PMAX // BASE):
        first = step * BASE
        last = first + BASE
        diagonal = work[first:last, first:last]
        both = jnp.concatenate([diagonal, eye, jnp.zeros((BASE, 128 - 2 * BASE), F32)], axis=1)
        for k in range(BASE - 1):
            column = jnp.where(small_rows > k, both[:, k : k + 1], 0.0)
            row = both[k : k + 1, :]
            both = both - column * (row / row[:, k : k + 1])
        pivot_values = jnp.sum(both[:, :BASE] * eye, axis=1, keepdims=True)
        inverse = both[:, BASE : 2 * BASE] / jnp.sqrt(pivot_values)
        strip = exact(inverse, work[first:last, :], NN)
        work[first:last, :] = strip
        if last < PMAX:
            update = exact(strip[:, :PMAX], strip, TN)
            work[last:, :] = work[last:, :] - update[last:, :]
    inverse_ref[...] = work[:, PMAX:]


def inverse_factor(pivots, columns):
    return pl.pallas_call(
        cholesky_kernel,
        grid=(1,),
        out_shape=jax.ShapeDtypeStruct((PMAX, PMAX), F32),
        in_specs=[pl.BlockSpec(memory_space=pltpu.SMEM), pl.BlockSpec((PMAX, PMAX), lambda j: (0, 0))],
        out_specs=pl.BlockSpec((PMAX, PMAX), lambda j: (0, 0)),
        scratch_shapes=[pltpu.VMEM((PMAX, 2 * PMAX), F32)],
        cost_estimate=pl.CostEstimate(flops=400_000_000, bytes_accessed=524288, transcendentals=0),
        name="inverse_factor",
    )(pivots, columns)


def gather_kernel(own_ref, all_ref, local_sem, send_sems, recv_sems):
    rank = lax.axis_index("grid")
    core = rank % 2
    chip = rank // 2
    x, y = chip // SIDE, chip % SIDE
    p = y + core * (x - y)
    s = x + core * (y - x)

    def device(dp, ds):
        pp, ss = (p + dp) % SIDE, (s + ds) % SIDE
        return 2 * (pp * (1 + 3 * core) + ss * (4 - 3 * core)) + core

    def rows(dp, ds, half=None):
        first = device(dp, ds) * ROWS
        if half is None:
            return pl.ds(pl.multiple_of(first, 64), ROWS)
        return pl.ds(pl.multiple_of(first + half * (ROWS // 2), 32), ROWS // 2)

    sems = (send_sems, recv_sems)
    sibling = {"grid": rank + 1 - 2 * core}
    p_up, p_down = {"grid": device(1, 0)}, {"grid": device(3, 0)}
    s_up, s_down = {"grid": device(0, 1)}, {"grid": device(0, 3)}
    greet((p_up, p_down, s_up, s_down, sibling))
    here = pltpu.make_async_copy(own_ref, all_ref.at[rows(0, 0)], local_sem)
    here.start()
    copies = []

    def send(index, where, target, source=None):
        copy = remote(all_ref.at[where] if source is None else source, all_ref.at[where], sems, index, target)
        copy.start()
        copies.append(copy)

    def arrived(index, where):
        remote(all_ref.at[where], all_ref.at[where], sems, index, sibling).wait_recv()

    def across(dp, ds, source=None):
        send(20 + 4 * dp + ds, rows(dp, ds), sibling, source)

    def sideways(dp):
        send(4 + dp, rows(dp, 0), s_up)
        send(8 + dp, rows(dp, 0), s_down)

    send(0, rows(0, 0), p_up, own_ref)
    send(1, rows(0, 0), p_down, own_ref)
    send(4, rows(0, 0), s_up, own_ref)
    send(8, rows(0, 0), s_down, own_ref)
    across(0, 0, own_ref)
    arrived(0, rows(3, 0))
    send(2, rows(3, 0, 0), p_up)
    sideways(3)
    across(3, 0)
    arrived(1, rows(1, 0))
    send(3, rows(1, 0, 1), p_down)
    sideways(1)
    across(1, 0)

    def pass_on(dp):
        arrived(4 + dp, rows(dp, 3))
        send(12 + dp, rows(dp, 3, 0), s_up)
        across(dp, 3)
        arrived(8 + dp, rows(dp, 1))
        send(16 + dp, rows(dp, 1, 1), s_down)
        across(dp, 1)

    pass_on(0)
    arrived(2, rows(2, 0, 0))
    arrived(3, rows(2, 0, 1))
    sideways(2)
    across(2, 0)
    for dp in (3, 1, 2):
        pass_on(dp)
    for dp in (0, 3, 1, 2):
        arrived(12 + dp, rows(dp, 2, 0))
        arrived(16 + dp, rows(dp, 2, 1))
        across(dp, 2)
    for copy in copies:
        copy.wait_send()
    for dp in range(SIDE):
        for ds in range(SIDE):
            chip_there = ((s + dp) % SIDE) * (4 - 3 * core) + ((p + ds) % SIDE) * (1 + 3 * core)
            first = (2 * chip_there + 1 - core) * ROWS
            arrived(20 + 4 * dp + ds, pl.ds(pl.multiple_of(first, 64), ROWS))
    here.wait()


def gather_rows(own, collective_id):
    return pl.pallas_call(
        gather_kernel,
        out_shape=jax.ShapeDtypeStruct((ORDER, PMAX), F32),
        in_specs=[pl.BlockSpec(memory_space=VMEM)],
        out_specs=pl.BlockSpec(memory_space=VMEM),
        scratch_shapes=[
            pltpu.SemaphoreType.DMA,
            pltpu.SemaphoreType.DMA((36,)),
            pltpu.SemaphoreType.DMA((36,)),
        ],
        compiler_params=pltpu.CompilerParams(collective_id=collective_id, has_side_effects=True),
        cost_estimate=pl.CostEstimate(flops=400_000_000, bytes_accessed=6_300_000, transcendentals=0),
        name="gather_rows",
    )(own)


def lead_kernel(pivots_ref, weight_ref, lead_ref, front_ref, out_ref, landing, send_sems, recv_sems):
    group = lax.axis_index("front")
    others = [{"front": (group + d) % SIDE} for d in range(1, SIDE)]
    greet(others)
    sems = (send_sems, recv_sems)
    copies = [remote(lead_ref.at[:, pl.ds(0, LEAD)], landing.at[d], sems, d, others[d]) for d in range(SIDE - 1)]
    for copy in copies:
        copy.start()
    pivots = pivots_ref[0]
    total = front_ref[...] + weight_ref[0] * lead_ref[:, :LEAD]
    for d in range(SIDE - 1):
        copies[d].wait()
        total = total + weight_ref[d + 1] * landing[d]
    columns = lax.broadcasted_iota(jnp.int32, (ROWS, LEAD), 1)
    out_ref[...] = jnp.where(columns < pivots, total, 0.0)


def lead_columns(pivots, weights, lead, front):
    smem = pl.BlockSpec(memory_space=pltpu.SMEM)
    return pl.pallas_call(
        lead_kernel,
        grid=(1,),
        out_shape=jax.ShapeDtypeStruct((ROWS, LEAD), F32),
        in_specs=[
            smem, smem,
            pl.BlockSpec((ROWS, WIDE), lambda j: (0, 0)),
            pl.BlockSpec((ROWS, LEAD), lambda j: (0, 0)),
        ],
        out_specs=pl.BlockSpec((ROWS, LEAD), lambda j: (0, 0)),
        scratch_shapes=[
            pltpu.VMEM((SIDE - 1, ROWS, LEAD), F32),
            pltpu.SemaphoreType.DMA((SIDE - 1,)),
            pltpu.SemaphoreType.DMA((SIDE - 1,)),
        ],
        compiler_params=pltpu.CompilerParams(collective_id=2, has_side_effects=True),
        cost_estimate=pl.CostEstimate(flops=200_000_000, bytes_accessed=1_000_000, transcendentals=0),
        name="lead_columns",
    )(pivots, weights, lead, front)


def fold_kernel(weight_ref, children_ref, sum_ref, mirror_ref):
    total = weight_ref[0] * children_ref[0, 0]
    for child in range(1, SIDE):
        total = total + weight_ref[child] * children_ref[child, 0]
    sum_ref[0] = total
    turned = total.T
    mirror_ref[0, 0] = turned[:ROWS]
    mirror_ref[0, 1] = turned[ROWS:]


def fold(weights, children):
    count = len(TURNED)
    return pl.pallas_call(
        fold_kernel,
        grid=(count,),
        out_shape=(
            jax.ShapeDtypeStruct((count, ROWS, WIDE), F32),
            jax.ShapeDtypeStruct((count, 2, ROWS, ROWS), F32),
        ),
        in_specs=[
            pl.BlockSpec(memory_space=pltpu.SMEM),
            pl.BlockSpec((SIDE, 1, ROWS, WIDE), lambda i: (0, i, 0, 0)),
        ],
        out_specs=(
            pl.BlockSpec((1, ROWS, WIDE), lambda i: (i, 0, 0)),
            pl.BlockSpec((1, 2, ROWS, ROWS), lambda i: (i, 0, 0, 0)),
        ),
        cost_estimate=pl.CostEstimate(flops=100_000_000, bytes_accessed=12_000_000, transcendentals=0),
        name="fold",
    )(weights, children)


def mirror_kernel(mirror_ref, landing_ref, send_sems, recv_sems):
    rank = lax.axis_index("grid")
    core = rank % 2
    chip = rank // 2
    sems = (send_sems, recv_sems)
    targets, sources = [], []
    for offset in TURNED:
        for k in range(2):
            targets.append({"grid": 2 * shifted(chip, offset) + k})
            sources.append({"grid": 2 * shifted(chip, offset, -1) + k})
    barrier = pltpu.get_barrier_semaphore()
    for device in sources:
        pl.semaphore_signal(barrier, inc=1, device_id=device, device_id_type=MESH)
    pl.semaphore_wait(barrier, len(targets))
    count = len(TURNED)
    copies = []
    for i in range(count):
        for k in range(2):
            copy = pltpu.make_async_remote_copy(
                src_ref=mirror_ref.at[i, k],
                dst_ref=landing_ref.at[i, core],
                send_sem=send_sems.at[2 * i + k],
                recv_sem=recv_sems.at[2 * i + core],
                device_id=targets[2 * i + k],
                device_id_type=MESH,
            )
            copy.start()
            copies.append(copy)
    for copy in copies:
        copy.wait_send()
    for i in range(count):
        for k in range(2):
            remote(mirror_ref.at[i, k], landing_ref.at[i, k], sems, 2 * i + k, targets[0]).wait_recv()


def mirror_blocks(mirror):
    count = len(TURNED)
    return pl.pallas_call(
        mirror_kernel,
        out_shape=jax.ShapeDtypeStruct((count, 2, ROWS, ROWS), F32),
        in_specs=[pl.BlockSpec(memory_space=VMEM)],
        out_specs=pl.BlockSpec(memory_space=VMEM),
        scratch_shapes=[pltpu.SemaphoreType.DMA((2 * count,)), pltpu.SemaphoreType.DMA((2 * count,))],
        compiler_params=pltpu.CompilerParams(collective_id=3, has_side_effects=True),
        cost_estimate=pl.CostEstimate(flops=400_000_000, bytes_accessed=5_000_000, transcendentals=0),
        name="mirror_blocks",
    )(mirror)


def turn_kernel(map_here, map_next, own_here, own_next, pair_here, pair_next, out_ref, window, places):
    core = lax.axis_index("grid") % 2
    block = pl.program_id(0)
    own = pl.ds(pl.multiple_of(core * ROWS, 64), ROWS)
    pair = pl.ds(pl.multiple_of((1 - core) * ROWS, 64), ROWS)
    window[own, :WIDE] = own_here[...]
    window[own, WIDE:] = own_next[...]
    window[pair, :WIDE] = pair_here[...]
    window[pair, WIDE:] = pair_next[...]
    places[:, :WIDE] = map_here[...]
    places[:, WIDE:] = map_next[...]
    lanes = pl.ds(pl.multiple_of(core * 128, 128), 512)
    first = block * WIDE + core * ROWS
    wanted = first + lax.broadcasted_iota(jnp.int32, (ROWS, 512), 0)
    one_hot = (wanted == places[:1, lanes]).astype(F32).astype(BF16)
    out_ref[0] = pick(one_hot, window[:, lanes], NT)


def turn(own, pair, places):
    here = lambda rows: pl.BlockSpec((rows, WIDE), lambda j: (0, j))
    after = lambda rows: pl.BlockSpec((rows, WIDE), lambda j: (0, jnp.minimum(j + 1, CHIPS - 1)))
    after_map = pl.BlockSpec((8, WIDE), lambda j: (0, j + 1))
    return pl.pallas_call(
        turn_kernel,
        grid=(CHIPS,),
        out_shape=jax.ShapeDtypeStruct((CHIPS, ROWS, WIDE), F32),
        in_specs=[here(8), after_map, here(ROWS), after(ROWS), here(ROWS), after(ROWS)],
        out_specs=pl.BlockSpec((1, ROWS, WIDE), lambda j: (j, 0, 0)),
        scratch_shapes=[pltpu.VMEM((WIDE, 2 * WIDE), F32), pltpu.VMEM((8, 2 * WIDE), jnp.int32)],
        cost_estimate=pl.CostEstimate(flops=400_000_000, bytes_accessed=15_000_000, transcendentals=0),
        name="turn",
    )(places, places, own, own, pair, pair)


def child_kernel(
    order_ref, map_here, map_next, map_own, map_after, here_ref, next_ref, own_ref, after_ref,
    inverse_ref, moved_here, moved_next, panel_ref, lead_ref, turned_ref, self_ref, weights, window, places,
):
    step = pl.program_id(0)
    grid_rank = lax.axis_index("grid")
    count = len(TURNED)

    @pl.when(step == 0)
    def _():
        inverse = inverse_ref[...]
        mine = pl.ds(pl.multiple_of((grid_rank % 2) * ROWS, 64), ROWS)
        panel_ref[...] = exact(own_ref[mine, :], inverse, NT)
        wanted = grid_rank * ROWS + lax.broadcasted_iota(jnp.int32, (ROWS, WIDE), 0)
        picked = pick((wanted == map_own[:1, :]).astype(F32).astype(BF16), own_ref[...], NN)
        picked += pick((wanted == map_after[:1, :]).astype(F32).astype(BF16), after_ref[...], NN)
        weights[...] = exact(exact(picked, inverse, NT), inverse, NN)

    w = weights[...]
    window[:, :WIDE] = moved_here[0] - product(w, here_ref[...], NT)
    window[:, WIDE:] = moved_next[0] - product(w, next_ref[...], NT)
    places[:, :WIDE] = map_here[...]
    places[:, WIDE:] = map_next[...]
    first = order_ref[step] * WIDE

    def columns(low, wide):
        wanted = first + low + lax.broadcasted_iota(jnp.int32, (wide, wide + 256), 0)
        one_hot = (wanted == places[:1, low : low + wide + 256]).astype(F32).astype(BF16)
        high, rest = split(window[:, low : low + wide + 256])
        return dot(high, one_hot, NT) + dot(rest, one_hot, NT)

    result = jnp.concatenate([columns(0, 256), columns(256, 128)], axis=1)

    @pl.when(step == 0)
    def _():
        lead_ref[...] = result

    @pl.when((step > 0) & (step <= count))
    def _():
        turned_ref[0] = result

    @pl.when(step > count)
    def _():
        self_ref[0] = result


def child_schur(order, places, columns, inverse, moved):
    last = CHIPS - 1
    count = len(TURNED)
    total = 1 + count + len(SELF)

    def block(shape, index):
        return pl.BlockSpec(shape, index)

    here = lambda i, order: order[i]
    after = lambda i, order: jnp.minimum(order[i] + 1, last)
    own = lambda i, order: order[total]
    own_after = lambda i, order: jnp.minimum(order[total] + 1, last)
    spec = pltpu.PrefetchScalarGridSpec(
        num_scalar_prefetch=1,
        grid=(total,),
        in_specs=[
            block((8, WIDE), lambda i, order: (0, order[i])),
            block((8, WIDE), lambda i, order: (0, order[i] + 1)),
            block((8, WIDE), lambda i, order: (0, order[total])),
            block((8, WIDE), lambda i, order: (0, order[total] + 1)),
            block((WIDE, PMAX), lambda i, order: (here(i, order), 0)),
            block((WIDE, PMAX), lambda i, order: (after(i, order), 0)),
            block((WIDE, PMAX), lambda i, order: (own(i, order), 0)),
            block((WIDE, PMAX), lambda i, order: (own_after(i, order), 0)),
            block((PMAX, PMAX), lambda i, order: (0, 0)),
            block((1, ROWS, WIDE), lambda i, order: (here(i, order), 0, 0)),
            block((1, ROWS, WIDE), lambda i, order: (after(i, order), 0, 0)),
        ],
        out_specs=(
            block((ROWS, PMAX), lambda i, order: (0, 0)),
            block((ROWS, WIDE), lambda i, order: (0, 0)),
            block((1, ROWS, WIDE), lambda i, order: (jnp.clip(i - 1, 0, count - 1), 0, 0)),
            block((1, ROWS, WIDE), lambda i, order: (jnp.clip(i - 1 - count, 0, SIDE - 1), 0, 0)),
        ),
        scratch_shapes=[
            pltpu.VMEM((ROWS, PMAX), F32),
            pltpu.VMEM((ROWS, 2 * WIDE), F32),
            pltpu.VMEM((8, 2 * WIDE), jnp.int32),
        ],
    )
    return pl.pallas_call(
        child_kernel,
        grid_spec=spec,
        out_shape=(
            jax.ShapeDtypeStruct((ROWS, PMAX), F32),
            jax.ShapeDtypeStruct((ROWS, WIDE), F32),
            jax.ShapeDtypeStruct((count, ROWS, WIDE), F32),
            jax.ShapeDtypeStruct((SIDE, ROWS, WIDE), F32),
        ),
        cost_estimate=pl.CostEstimate(flops=400_000_000, bytes_accessed=20_000_000, transcendentals=0),
        name="child_schur",
    )(order, places, places, places, places, columns, columns, columns, columns, inverse, moved, moved)


def parent_kernel(
    order_ref, pivots_ref, weight_ref, own_ref, here_ref, inverse_ref, self_ref, sum_ref, mirror_ref, front_ref,
    panel_ref, schur_ref, weights,
):
    step = pl.program_id(0)
    grid_rank = lax.axis_index("grid")
    count = len(TURNED)

    @pl.when(step == 0)
    def _():
        inverse = inverse_ref[...]
        panel = exact(own_ref[...], inverse, NT)
        panel_ref[...] = panel
        weights[...] = exact(panel, inverse, NN)

    total = front_ref[...] - product(weights[...], here_ref[...], NT)
    pivots = pivots_ref[0]
    rows = grid_rank * ROWS + lax.broadcasted_iota(jnp.int32, (ROWS, WIDE), 0)
    columns = order_ref[step] * WIDE + lax.broadcasted_iota(jnp.int32, (ROWS, WIDE), 1)
    keep = (rows >= pivots) & (columns >= pivots)

    @pl.when(step < count)
    def _():
        schur_ref[...] = jnp.where(keep, total + sum_ref[0], 0.0)

    @pl.when((step >= count) & (step < 2 * count))
    def _():
        mirror = jnp.concatenate([mirror_ref[0, 0], mirror_ref[0, 1]], axis=1)
        schur_ref[...] = jnp.where(keep, total + mirror, 0.0)

    @pl.when(step >= 2 * count)
    def _():
        result = total
        for child in range(SIDE):
            result = result + weight_ref[child] * self_ref[child, 0]
        schur_ref[...] = jnp.where(keep, result, 0.0)


def parent_schur(order, pivots, weights, own, columns, inverse, selves, sums, mirror, front):
    smem = pl.BlockSpec(memory_space=pltpu.SMEM)
    count = len(TURNED)
    spec = pltpu.PrefetchScalarGridSpec(
        num_scalar_prefetch=1,
        grid=(CHIPS,),
        in_specs=[
            smem,
            smem,
            pl.BlockSpec((ROWS, PMAX), lambda i, order: (0, 0)),
            pl.BlockSpec((WIDE, PMAX), lambda i, order: (order[i], 0)),
            pl.BlockSpec((PMAX, PMAX), lambda i, order: (0, 0)),
            pl.BlockSpec((SIDE, 1, ROWS, WIDE), lambda i, order: (0, jnp.clip(i - 2 * count, 0, SIDE - 1), 0, 0)),
            pl.BlockSpec((1, ROWS, WIDE), lambda i, order: (jnp.clip(i, 0, count - 1), 0, 0)),
            pl.BlockSpec((1, 2, ROWS, ROWS), lambda i, order: (jnp.clip(i - count, 0, count - 1), 0, 0, 0)),
            pl.BlockSpec((ROWS, WIDE), lambda i, order: (0, order[i])),
        ],
        out_specs=(
            pl.BlockSpec((ROWS, PMAX), lambda i, order: (0, 0)),
            pl.BlockSpec((ROWS, WIDE), lambda i, order: (0, order[i])),
        ),
        scratch_shapes=[pltpu.VMEM((ROWS, PMAX), F32)],
    )
    return pl.pallas_call(
        parent_kernel,
        grid_spec=spec,
        out_shape=(jax.ShapeDtypeStruct((ROWS, PMAX), F32), jax.ShapeDtypeStruct((ROWS, ORDER), F32)),
        cost_estimate=pl.CostEstimate(flops=400_000_000, bytes_accessed=30_000_000, transcendentals=0),
        name="parent_schur",
    )(order, pivots, weights, own, columns, inverse, selves, sums, mirror, front)


def on_device(child_fronts, parent_fronts, child_maps, parent_of, child_pivots, parent_pivots):
    front_group = lax.axis_index("front")
    chip = lax.axis_index("grid") // 2
    front_rows = child_fronts[0]
    child_map = child_maps[front_group]
    pivots = child_pivots[front_group]
    upper_pivots = parent_pivots[front_group]
    weights = (parent_of == front_group).astype(F32)
    groups = (front_group - jnp.arange(SIDE, dtype=jnp.int32)) % SIDE
    lead_weights = (parent_of[groups] == front_group).astype(F32)
    turned_chips = [shifted(chip, offset) for offset in TURNED]
    mirror_chips = [shifted(chip, offset, -1) for offset in TURNED]
    self_chips = [shifted(chip, offset) for offset in SELF]
    child_order = jnp.stack([0 * chip] + turned_chips + self_chips + [chip]).astype(jnp.int32)
    parent_order = jnp.stack(turned_chips + mirror_chips + self_chips).astype(jnp.int32)

    pair = lax.ppermute(front_rows, "grid", [(g, g ^ 1) for g in range(2 * CHIPS)])
    position = jnp.arange(ORDER, dtype=jnp.int32)
    line = jnp.where(position >= pivots, child_map, -1)
    line = jnp.pad(line, (0, 2 * WIDE), constant_values=-1)
    places = jnp.broadcast_to(line[None], (8, line.shape[0]))
    turned = turn(front_rows, pair, places)
    same_core = [[2 * c + k for c in range(CHIPS)] for k in range(2)]
    moved = lax.all_to_all(turned, "grid", 0, 0, axis_index_groups=same_core)

    own = jnp.where(position[:PMAX] < pivots, front_rows[:, :PMAX], 0.0)
    columns = gather_rows(own, 0)
    inverse = inverse_factor(pivots[None], columns)
    panel_rows, lead, turned_part, self_part = child_schur(child_order, places, columns, inverse, moved)

    upper_own = lead_columns(upper_pivots[None], lead_weights, lead, parent_fronts[0])
    turned_all = lax.all_gather(turned_part, "front", axis=0)
    self_all = lax.all_gather(self_part, "front", axis=0)
    upper_columns = gather_rows(upper_own, 1)
    upper_inverse = inverse_factor(upper_pivots[None], upper_columns)
    sums, mirror = fold(weights, turned_all)
    landed = mirror_blocks(mirror)
    upper_panel, upper_schur = parent_schur(
        parent_order, upper_pivots[None], weights, upper_own, upper_columns, upper_inverse,
        self_all, sums, landed, parent_fronts[0],
    )
    return (panel_rows[None], upper_panel[None], upper_schur[None])


def solution(mesh):
    in_specs = (P("front", "grid", None), P("front", "grid", None), P(), P(), P(), P())
    out_specs = (P("front", "grid", None), P("front", "grid", None), P("front", "grid", None))
    return jax.shard_map(
        on_device, mesh=mesh, in_specs=in_specs, out_specs=out_specs, check_vma=False
    )
```

```python
import functools

import jax
import jax.numpy as jnp
from jax import lax
from jax.experimental import pallas as pl
from jax.experimental.pallas import tpu as pltpu
from jax.sharding import PartitionSpec as P

PMAX = 256
CHIPS = 16
SIDE = 4
ROWS = 192
WIDE = 384
ORDER = 6144
BASE = 32
GROUP = 8
LEAD = 256
MESH = pl.DeviceIdType.MESH
SELF = ((0, 0), (0, 2), (2, 0), (2, 2))
TURNED = ((0, 1), (1, 0), (3, 3), (3, 1), (1, 2), (2, 3))
F32 = jnp.float32
BF16 = jnp.bfloat16
VMEM = pltpu.VMEM
NT = (((1,), (1,)), ((), ()))
NN = (((1,), (0,)), ((), ()))
TN = (((0,), (0,)), ((), ()))


def dot(a, b, dims):
    return lax.dot_general(a, b, dims, preferred_element_type=F32)


def split(a):
    high = a.astype(BF16)
    low = (a - high.astype(F32)).astype(BF16)
    return high, low


def product(a, b, dims):
    a_high, a_low = split(a)
    b_high, b_low = split(b)
    return dot(a_high, b_high, dims) + (dot(a_high, b_low, dims) + dot(a_low, b_high, dims))


def pick(one_hot, a, dims):
    a_high, a_low = split(a)
    return dot(one_hot, a_high, dims) + dot(one_hot, a_low, dims)


def exact(a, b, dims):
    return lax.dot_general(a, b, dims, precision=lax.Precision.HIGHEST, preferred_element_type=F32)


def shifted(chip, offset, sign=1):
    x = (chip // SIDE + sign * offset[0] + SIDE) % SIDE
    y = (chip % SIDE + sign * offset[1] + SIDE) % SIDE
    return x * SIDE + y


def remote(src, dst, sems, index, device):
    return pltpu.make_async_remote_copy(
        src_ref=src, dst_ref=dst, send_sem=sems[0].at[index], recv_sem=sems[1].at[index],
        device_id=device, device_id_type=MESH,
    )


def greet(devices):
    barrier = pltpu.get_barrier_semaphore()
    for device in devices:
        pl.semaphore_signal(barrier, inc=1, device_id=device, device_id_type=MESH)
    pl.semaphore_wait(barrier, len(devices))


def cholesky_kernel(pivots_ref, block_ref, inverse_ref, work):
    rows = lax.broadcasted_iota(jnp.int32, (PMAX, PMAX), 0)
    columns = lax.broadcasted_iota(jnp.int32, (PMAX, PMAX), 1)
    same = (rows == columns).astype(F32)
    pivots = pivots_ref[0]
    work[:, :PMAX] = jnp.where((rows < pivots) & (columns < pivots), block_ref[...], same)
    work[:, PMAX:] = same
    small_rows = lax.broadcasted_iota(jnp.int32, (BASE, 1), 0)
    eye_rows = lax.broadcasted_iota(jnp.int32, (BASE, BASE), 0)
    eye_columns = lax.broadcasted_iota(jnp.int32, (BASE, BASE), 1)
    eye = (eye_rows == eye_columns).astype(F32)
    for step in range(PMAX // BASE):
        first = step * BASE
        last = first + BASE
        diagonal = work[first:last, first:last]
        both = jnp.concatenate([diagonal, eye, jnp.zeros((BASE, 128 - 2 * BASE), F32)], axis=1)
        for group in range(0, BASE, GROUP):
            columns_of = [jnp.broadcast_to(both[:, group + i : group + i + 1], (BASE, 128)) for i in range(GROUP)]
            rows_of = [both[group + i : group + i + 1, :] for i in range(GROUP)]
            for i in range(GROUP):
                k = group + i
                below = jnp.where(small_rows > k, columns_of[i], 0.0)
                inverse_pivot = 1.0 / columns_of[i][k : k + 1, :]
                scaled = rows_of[i] * inverse_pivot
                for j in range(i + 1, GROUP):
                    entry = columns_of[i][group + j : group + j + 1, :]
                    columns_of[j] = columns_of[j] - below * (entry * inverse_pivot)
                    rows_of[j] = rows_of[j] - entry * scaled
                both = both - below * scaled
        pivot_values = jnp.sum(both[:, :BASE] * eye, axis=1, keepdims=True)
        inverse = both[:, BASE : 2 * BASE] / jnp.sqrt(pivot_values)
        strip = exact(inverse, work[first:last, :], NN)
        work[first:last, :] = strip
        if last < PMAX:
            update = exact(strip[:, :PMAX], strip, TN)
            work[last:, :] = work[last:, :] - update[last:, :]
    inverse_ref[...] = jnp.where(rows < pivots, work[:, PMAX:], 0.0)


def inverse_factor(pivots, columns):
    return pl.pallas_call(
        cholesky_kernel,
        grid=(1,),
        out_shape=jax.ShapeDtypeStruct((PMAX, PMAX), F32),
        in_specs=[pl.BlockSpec(memory_space=pltpu.SMEM), pl.BlockSpec((PMAX, PMAX), lambda j: (0, 0))],
        out_specs=pl.BlockSpec((PMAX, PMAX), lambda j: (0, 0)),
        scratch_shapes=[pltpu.VMEM((PMAX, 2 * PMAX), F32)],
        cost_estimate=pl.CostEstimate(flops=400_000_000, bytes_accessed=524288, transcendentals=0),
        name="inverse_factor",
    )(pivots, columns)


def gather_stages(own_ref, all_ref, local_sem, send_sems, recv_sems):
    rank = lax.axis_index("grid")
    core = rank % 2
    chip = rank // 2
    x, y = chip // SIDE, chip % SIDE
    p = y + core * (x - y)
    s = x + core * (y - x)

    def device(dp, ds):
        pp, ss = (p + dp) % SIDE, (s + ds) % SIDE
        return 2 * (pp * (1 + 3 * core) + ss * (4 - 3 * core)) + core

    def rows(dp, ds, half=None):
        first = device(dp, ds) * ROWS
        if half is None:
            return pl.ds(pl.multiple_of(first, 64), ROWS)
        return pl.ds(pl.multiple_of(first + half * (ROWS // 2), 32), ROWS // 2)

    sems = (send_sems, recv_sems)
    sibling = {"grid": rank + 1 - 2 * core}
    p_up, p_down = {"grid": device(1, 0)}, {"grid": device(3, 0)}
    s_up, s_down = {"grid": device(0, 1)}, {"grid": device(0, 3)}
    greet((p_up, p_down, s_up, s_down, sibling))
    here = pltpu.make_async_copy(own_ref, all_ref.at[rows(0, 0)], local_sem)
    here.start()
    copies = []

    def send(index, where, target, source=None):
        copy = remote(all_ref.at[where] if source is None else source, all_ref.at[where], sems, index, target)
        copy.start()
        copies.append(copy)

    def arrived(index, where):
        remote(all_ref.at[where], all_ref.at[where], sems, index, sibling).wait_recv()

    def across(dp, ds, source=None):
        send(20 + 4 * dp + ds, rows(dp, ds), sibling, source)

    def sideways(dp):
        send(4 + dp, rows(dp, 0), s_up)
        send(8 + dp, rows(dp, 0), s_down)

    def begin():
        send(0, rows(0, 0), p_up, own_ref)
        send(1, rows(0, 0), p_down, own_ref)
        send(4, rows(0, 0), s_up, own_ref)
        send(8, rows(0, 0), s_down, own_ref)
        across(0, 0, own_ref)

    def from_below():
        arrived(0, rows(3, 0))
        send(2, rows(3, 0, 0), p_up)
        sideways(3)
        across(3, 0)

    def from_above():
        arrived(1, rows(1, 0))
        send(3, rows(1, 0, 1), p_down)
        sideways(1)
        across(1, 0)

    def pass_on(dp):
        arrived(4 + dp, rows(dp, 3))
        send(12 + dp, rows(dp, 3, 0), s_up)
        across(dp, 3)
        arrived(8 + dp, rows(dp, 1))
        send(16 + dp, rows(dp, 1, 1), s_down)
        across(dp, 1)

    def opposite():
        arrived(2, rows(2, 0, 0))
        arrived(3, rows(2, 0, 1))
        sideways(2)
        across(2, 0)

    def complete(dp):
        arrived(12 + dp, rows(dp, 2, 0))
        arrived(16 + dp, rows(dp, 2, 1))
        across(dp, 2)

    def finish():
        for copy in copies:
            copy.wait_send()
        for dp in range(SIDE):
            for ds in range(SIDE):
                chip_there = ((s + dp) % SIDE) * (4 - 3 * core) + ((p + ds) % SIDE) * (1 + 3 * core)
                first = (2 * chip_there + 1 - core) * ROWS
                arrived(20 + 4 * dp + ds, pl.ds(pl.multiple_of(first, 64), ROWS))
        here.wait()

    steps = [begin, from_below, from_above, functools.partial(pass_on, 0), opposite]
    steps += [functools.partial(pass_on, dp) for dp in (3, 1, 2)]
    steps += [functools.partial(complete, dp) for dp in (0, 3, 1, 2)]
    return steps + [finish]


def gather_kernel(own_ref, all_ref, local_sem, send_sems, recv_sems):
    for step in gather_stages(own_ref, all_ref, local_sem, send_sems, recv_sems):
        step()


def gather_rows(own, collective_id):
    return pl.pallas_call(
        gather_kernel,
        out_shape=jax.ShapeDtypeStruct((ORDER, PMAX), F32),
        in_specs=[pl.BlockSpec(memory_space=VMEM)],
        out_specs=pl.BlockSpec(memory_space=VMEM),
        scratch_shapes=[
            pltpu.SemaphoreType.DMA,
            pltpu.SemaphoreType.DMA((36,)),
            pltpu.SemaphoreType.DMA((36,)),
        ],
        compiler_params=pltpu.CompilerParams(collective_id=collective_id, has_side_effects=True),
        cost_estimate=pl.CostEstimate(flops=400_000_000, bytes_accessed=6_300_000, transcendentals=0),
        name="gather_rows",
    )(own)


def lead_kernel(weight_ref, lead_ref, front_ref, out_ref, landing, send_sems, recv_sems):
    group = lax.axis_index("front")
    others = [{"front": (group + d) % SIDE} for d in range(1, SIDE)]
    greet(others)
    sems = (send_sems, recv_sems)
    copies = [remote(lead_ref.at[:, pl.ds(0, LEAD)], landing.at[d], sems, d, others[d]) for d in range(SIDE - 1)]
    for copy in copies:
        copy.start()
    total = front_ref[...] + weight_ref[0] * lead_ref[:, :LEAD]
    for d in range(SIDE - 1):
        copies[d].wait()
        total = total + weight_ref[d + 1] * landing[d]
    out_ref[...] = total


def lead_columns(weights, lead, front):
    smem = pl.BlockSpec(memory_space=pltpu.SMEM)
    return pl.pallas_call(
        lead_kernel,
        grid=(1,),
        out_shape=jax.ShapeDtypeStruct((ROWS, LEAD), F32),
        in_specs=[
            smem,
            pl.BlockSpec((ROWS, WIDE), lambda j: (0, 0)),
            pl.BlockSpec((ROWS, LEAD), lambda j: (0, 0)),
        ],
        out_specs=pl.BlockSpec((ROWS, LEAD), lambda j: (0, 0)),
        scratch_shapes=[
            pltpu.VMEM((SIDE - 1, ROWS, LEAD), F32),
            pltpu.SemaphoreType.DMA((SIDE - 1,)),
            pltpu.SemaphoreType.DMA((SIDE - 1,)),
        ],
        compiler_params=pltpu.CompilerParams(collective_id=2, has_side_effects=True),
        cost_estimate=pl.CostEstimate(flops=200_000_000, bytes_accessed=1_000_000, transcendentals=0),
        name="lead_columns",
    )(weights, lead, front)


def fold_kernel(weight_ref, children_ref, sum_ref, mirror_ref):
    total = weight_ref[0] * children_ref[0, 0]
    for child in range(1, SIDE):
        total = total + weight_ref[child] * children_ref[child, 0]
    sum_ref[0] = total
    turned = total.T
    mirror_ref[0, 0] = turned[:ROWS]
    mirror_ref[0, 1] = turned[ROWS:]


def fold(weights, children):
    count = len(TURNED)
    return pl.pallas_call(
        fold_kernel,
        grid=(count,),
        out_shape=(
            jax.ShapeDtypeStruct((count, ROWS, WIDE), F32),
            jax.ShapeDtypeStruct((count, 2, ROWS, ROWS), F32),
        ),
        in_specs=[
            pl.BlockSpec(memory_space=pltpu.SMEM),
            pl.BlockSpec((SIDE, 1, ROWS, WIDE), lambda i: (0, i, 0, 0)),
        ],
        out_specs=(
            pl.BlockSpec((1, ROWS, WIDE), lambda i: (i, 0, 0)),
            pl.BlockSpec((1, 2, ROWS, ROWS), lambda i: (i, 0, 0, 0)),
        ),
        cost_estimate=pl.CostEstimate(flops=100_000_000, bytes_accessed=12_000_000, transcendentals=0),
        name="fold",
    )(weights, children)


def mirror_kernel(mirror_ref, landing_ref, send_sems, recv_sems):
    rank = lax.axis_index("grid")
    core = rank % 2
    chip = rank // 2
    sems = (send_sems, recv_sems)
    targets, sources = [], []
    for offset in TURNED:
        for k in range(2):
            targets.append({"grid": 2 * shifted(chip, offset) + k})
            sources.append({"grid": 2 * shifted(chip, offset, -1) + k})
    barrier = pltpu.get_barrier_semaphore()
    for device in sources:
        pl.semaphore_signal(barrier, inc=1, device_id=device, device_id_type=MESH)
    pl.semaphore_wait(barrier, len(targets))
    count = len(TURNED)
    copies = []
    for i in range(count):
        for k in range(2):
            copy = pltpu.make_async_remote_copy(
                src_ref=mirror_ref.at[i, k],
                dst_ref=landing_ref.at[i, core],
                send_sem=send_sems.at[2 * i + k],
                recv_sem=recv_sems.at[2 * i + core],
                device_id=targets[2 * i + k],
                device_id_type=MESH,
            )
            copy.start()
            copies.append(copy)
    for copy in copies:
        copy.wait_send()
    for i in range(count):
        for k in range(2):
            remote(mirror_ref.at[i, k], landing_ref.at[i, k], sems, 2 * i + k, targets[0]).wait_recv()


def mirror_blocks(mirror):
    count = len(TURNED)
    return pl.pallas_call(
        mirror_kernel,
        out_shape=jax.ShapeDtypeStruct((count, 2, ROWS, ROWS), F32),
        in_specs=[pl.BlockSpec(memory_space=VMEM)],
        out_specs=pl.BlockSpec(memory_space=VMEM),
        scratch_shapes=[pltpu.SemaphoreType.DMA((2 * count,)), pltpu.SemaphoreType.DMA((2 * count,))],
        compiler_params=pltpu.CompilerParams(collective_id=3, has_side_effects=True),
        cost_estimate=pl.CostEstimate(flops=400_000_000, bytes_accessed=5_000_000, transcendentals=0),
        name="mirror_blocks",
    )(mirror)


def front_kernel(
    places_ref, rows_ref, own_ref, all_ref, turned_ref, both, local_sem, send_sems, recv_sems, own_sems, out_sems, in_sems
):
    rank = lax.axis_index("grid")
    core = rank % 2
    steps = gather_stages(own_ref, all_ref, local_sem, send_sems, recv_sems)
    sibling = {"grid": rank + 1 - 2 * core}
    mine = pl.ds(pl.multiple_of(core * ROWS, 64), ROWS)

    def local(j):
        lanes = pl.ds(pl.multiple_of(j * WIDE, 128), WIDE)
        return pltpu.make_async_copy(rows_ref.at[:, lanes], both.at[mine, lanes], own_sems.at[j])

    def pair(j):
        lanes = pl.ds(pl.multiple_of(j * WIDE, 128), WIDE)
        return pltpu.make_async_remote_copy(
            src_ref=rows_ref.at[:, lanes], dst_ref=both.at[mine, lanes],
            send_sem=out_sems.at[j], recv_sem=in_sems.at[j], device_id=sibling, device_id_type=MESH,
        )

    steps[0]()
    for j in range(CHIPS):
        pair(j).start()
        local(j).start()

    def here(j):
        local(j).wait()
        pair(j).wait()

    def work(j, carry):
        @pl.when(j < CHIPS - 1)
        def _():
            here(j + 1)

        first = j * WIDE + core * ROWS
        start = jnp.minimum(j * WIDE + core * 128, ORDER - 512)
        lanes = pl.ds(pl.multiple_of(start, 128), 512)
        wanted = first + lax.broadcasted_iota(jnp.int32, (ROWS, 512), 0)
        one_hot = (wanted == places_ref[:1, lanes]).astype(F32).astype(BF16)
        turned_ref[j] = pick(one_hot, both[:, lanes], NT)
        return carry

    here(0)
    done = 0
    rest = steps[1:-1]
    for index, step in enumerate(rest):
        until = (CHIPS * (index + 1)) // len(rest)
        lax.fori_loop(done, until, work, 0)
        done = until
        step()
    steps[-1]()


def front(rows, places):
    return pl.pallas_call(
        front_kernel,
        grid=(1,),
        out_shape=(
            jax.ShapeDtypeStruct((ORDER, PMAX), F32),
            jax.ShapeDtypeStruct((CHIPS, ROWS, WIDE), F32),
        ),
        in_specs=[
            pl.BlockSpec(places.shape, lambda i: (0, 0)),
            pl.BlockSpec(memory_space=pl.ANY),
            pl.BlockSpec((ROWS, PMAX), lambda i: (0, 0)),
        ],
        out_specs=(
            pl.BlockSpec((ORDER, PMAX), lambda i: (0, 0)),
            pl.BlockSpec((CHIPS, ROWS, WIDE), lambda i: (0, 0, 0)),
        ),
        scratch_shapes=[
            pltpu.VMEM((WIDE, ORDER), F32),
            pltpu.SemaphoreType.DMA,
            pltpu.SemaphoreType.DMA((36,)),
            pltpu.SemaphoreType.DMA((36,)),
            pltpu.SemaphoreType.DMA((CHIPS,)),
            pltpu.SemaphoreType.DMA((CHIPS,)),
            pltpu.SemaphoreType.DMA((CHIPS,)),
        ],
        compiler_params=pltpu.CompilerParams(collective_id=0, has_side_effects=True),
        cost_estimate=pl.CostEstimate(flops=400_000_000, bytes_accessed=25_000_000, transcendentals=0),
        name="front",
    )(places, rows, rows)


def child_kernel(
    order_ref, map_here, map_next, map_own, map_after, here_ref, next_ref, own_ref, after_ref,
    inverse_ref, moved_here, moved_next, panel_ref, lead_ref, turned_ref, self_ref, weights, window, places,
):
    step = pl.program_id(0)
    grid_rank = lax.axis_index("grid")
    count = len(TURNED)

    @pl.when(step == 0)
    def _():
        inverse = inverse_ref[...]
        mine = pl.ds(pl.multiple_of((grid_rank % 2) * ROWS, 64), ROWS)
        panel_ref[...] = exact(own_ref[mine, :], inverse, NT)
        wanted = grid_rank * ROWS + lax.broadcasted_iota(jnp.int32, (ROWS, WIDE), 0)
        picked = pick((wanted == map_own[:1, :]).astype(F32).astype(BF16), own_ref[...], NN)
        picked += pick((wanted == map_after[:1, :]).astype(F32).astype(BF16), after_ref[...], NN)
        weights[...] = exact(exact(picked, inverse, NT), inverse, NN)

    w = weights[...]
    window[:, :WIDE] = moved_here[0] - product(w, here_ref[...], NT)
    window[:, WIDE:] = moved_next[0] - product(w, next_ref[...], NT)
    places[:, :WIDE] = map_here[...]
    places[:, WIDE:] = map_next[...]
    first = order_ref[step] * WIDE

    def columns(low, wide):
        wanted = first + low + lax.broadcasted_iota(jnp.int32, (wide, wide + 256), 0)
        one_hot = (wanted == places[:1, low : low + wide + 256]).astype(F32).astype(BF16)
        high, rest = split(window[:, low : low + wide + 256])
        return dot(high, one_hot, NT) + dot(rest, one_hot, NT)

    result = jnp.concatenate([columns(0, 256), columns(256, 128)], axis=1)

    @pl.when(step == 0)
    def _():
        lead_ref[...] = result

    @pl.when((step > 0) & (step <= count))
    def _():
        turned_ref[0] = result

    @pl.when(step > count)
    def _():
        self_ref[0] = result


def child_schur(order, places, columns, inverse, moved):
    last = CHIPS - 1
    count = len(TURNED)
    total = 1 + count + len(SELF)

    def block(shape, index):
        return pl.BlockSpec(shape, index)

    here = lambda i, order: order[i]
    after = lambda i, order: jnp.minimum(order[i] + 1, last)
    own = lambda i, order: order[total]
    own_after = lambda i, order: jnp.minimum(order[total] + 1, last)
    spec = pltpu.PrefetchScalarGridSpec(
        num_scalar_prefetch=1,
        grid=(total,),
        in_specs=[
            block((8, WIDE), lambda i, order: (0, order[i])),
            block((8, WIDE), lambda i, order: (0, order[i] + 1)),
            block((8, WIDE), lambda i, order: (0, order[total])),
            block((8, WIDE), lambda i, order: (0, order[total] + 1)),
            block((WIDE, PMAX), lambda i, order: (here(i, order), 0)),
            block((WIDE, PMAX), lambda i, order: (after(i, order), 0)),
            block((WIDE, PMAX), lambda i, order: (own(i, order), 0)),
            block((WIDE, PMAX), lambda i, order: (own_after(i, order), 0)),
            block((PMAX, PMAX), lambda i, order: (0, 0)),
            block((1, ROWS, WIDE), lambda i, order: (here(i, order), 0, 0)),
            block((1, ROWS, WIDE), lambda i, order: (after(i, order), 0, 0)),
        ],
        out_specs=(
            block((ROWS, PMAX), lambda i, order: (0, 0)),
            block((ROWS, WIDE), lambda i, order: (0, 0)),
            block((1, ROWS, WIDE), lambda i, order: (jnp.clip(i - 1, 0, count - 1), 0, 0)),
            block((1, ROWS, WIDE), lambda i, order: (jnp.clip(i - 1 - count, 0, SIDE - 1), 0, 0)),
        ),
        scratch_shapes=[
            pltpu.VMEM((ROWS, PMAX), F32),
            pltpu.VMEM((ROWS, 2 * WIDE), F32),
            pltpu.VMEM((8, 2 * WIDE), jnp.int32),
        ],
    )
    return pl.pallas_call(
        child_kernel,
        grid_spec=spec,
        out_shape=(
            jax.ShapeDtypeStruct((ROWS, PMAX), F32),
            jax.ShapeDtypeStruct((ROWS, WIDE), F32),
            jax.ShapeDtypeStruct((count, ROWS, WIDE), F32),
            jax.ShapeDtypeStruct((SIDE, ROWS, WIDE), F32),
        ),
        cost_estimate=pl.CostEstimate(flops=400_000_000, bytes_accessed=20_000_000, transcendentals=0),
        name="child_schur",
    )(order, places, places, places, places, columns, columns, columns, columns, inverse, moved, moved)


def parent_kernel(
    order_ref, pivots_ref, weight_ref, own_ref, here_ref, inverse_ref, self_ref, sum_ref, mirror_ref, front_ref,
    panel_ref, schur_ref, weights,
):
    step = pl.program_id(0)
    grid_rank = lax.axis_index("grid")
    count = len(TURNED)

    @pl.when(step == 0)
    def _():
        inverse = inverse_ref[...]
        panel = exact(own_ref[...], inverse, NT)
        panel_ref[...] = panel
        weights[...] = exact(panel, inverse, NN)

    total = front_ref[...] - product(weights[...], here_ref[...], NT)
    pivots = pivots_ref[0]
    rows = grid_rank * ROWS + lax.broadcasted_iota(jnp.int32, (ROWS, WIDE), 0)
    columns = order_ref[step] * WIDE + lax.broadcasted_iota(jnp.int32, (ROWS, WIDE), 1)
    keep = (rows >= pivots) & (columns >= pivots)

    @pl.when(step < count)
    def _():
        schur_ref[...] = jnp.where(keep, total + sum_ref[0], 0.0)

    @pl.when((step >= count) & (step < 2 * count))
    def _():
        mirror = jnp.concatenate([mirror_ref[0, 0], mirror_ref[0, 1]], axis=1)
        schur_ref[...] = jnp.where(keep, total + mirror, 0.0)

    @pl.when(step >= 2 * count)
    def _():
        result = total
        for child in range(SIDE):
            result = result + weight_ref[child] * self_ref[child, 0]
        schur_ref[...] = jnp.where(keep, result, 0.0)


def parent_schur(order, pivots, weights, own, columns, inverse, selves, sums, mirror, front):
    smem = pl.BlockSpec(memory_space=pltpu.SMEM)
    count = len(TURNED)
    spec = pltpu.PrefetchScalarGridSpec(
        num_scalar_prefetch=1,
        grid=(CHIPS,),
        in_specs=[
            smem,
            smem,
            pl.BlockSpec((ROWS, PMAX), lambda i, order: (0, 0)),
            pl.BlockSpec((WIDE, PMAX), lambda i, order: (order[i], 0)),
            pl.BlockSpec((PMAX, PMAX), lambda i, order: (0, 0)),
            pl.BlockSpec((SIDE, 1, ROWS, WIDE), lambda i, order: (0, jnp.clip(i - 2 * count, 0, SIDE - 1), 0, 0)),
            pl.BlockSpec((1, ROWS, WIDE), lambda i, order: (jnp.clip(i, 0, count - 1), 0, 0)),
            pl.BlockSpec((1, 2, ROWS, ROWS), lambda i, order: (jnp.clip(i - count, 0, count - 1), 0, 0, 0)),
            pl.BlockSpec((ROWS, WIDE), lambda i, order: (0, order[i])),
        ],
        out_specs=(
            pl.BlockSpec((ROWS, PMAX), lambda i, order: (0, 0)),
            pl.BlockSpec((ROWS, WIDE), lambda i, order: (0, order[i])),
        ),
        scratch_shapes=[pltpu.VMEM((ROWS, PMAX), F32)],
    )
    return pl.pallas_call(
        parent_kernel,
        grid_spec=spec,
        out_shape=(jax.ShapeDtypeStruct((ROWS, PMAX), F32), jax.ShapeDtypeStruct((ROWS, ORDER), F32)),
        cost_estimate=pl.CostEstimate(flops=400_000_000, bytes_accessed=30_000_000, transcendentals=0),
        name="parent_schur",
    )(order, pivots, weights, own, columns, inverse, selves, sums, mirror, front)


def on_device(child_fronts, parent_fronts, child_maps, parent_of, child_pivots, parent_pivots):
    front_group = lax.axis_index("front")
    chip = lax.axis_index("grid") // 2
    front_rows = child_fronts[0]
    child_map = child_maps[front_group]
    pivots = child_pivots[front_group]
    upper_pivots = parent_pivots[front_group]
    weights = (parent_of == front_group).astype(F32)
    groups = (front_group - jnp.arange(SIDE, dtype=jnp.int32)) % SIDE
    lead_weights = (parent_of[groups] == front_group).astype(F32)
    turned_chips = [shifted(chip, offset) for offset in TURNED]
    mirror_chips = [shifted(chip, offset, -1) for offset in TURNED]
    self_chips = [shifted(chip, offset) for offset in SELF]
    child_order = jnp.stack([0 * chip] + turned_chips + self_chips + [chip]).astype(jnp.int32)
    parent_order = jnp.stack(turned_chips + mirror_chips + self_chips).astype(jnp.int32)

    position = jnp.arange(ORDER, dtype=jnp.int32)
    line = jnp.where(position >= pivots, child_map, -1)
    line = jnp.pad(line, (0, 2 * WIDE), constant_values=-1)
    places = jnp.broadcast_to(line[None], (8, line.shape[0]))
    columns, turned = front(front_rows, places)
    same_core = [[2 * c + k for c in range(CHIPS)] for k in range(2)]
    moved = lax.all_to_all(turned, "grid", 0, 0, axis_index_groups=same_core)

    inverse = inverse_factor(pivots[None], columns)
    panel_rows, lead, turned_part, self_part = child_schur(child_order, places, columns, inverse, moved)

    upper_own = lead_columns(lead_weights, lead, parent_fronts[0])
    turned_all = lax.all_gather(turned_part, "front", axis=0)
    self_all = lax.all_gather(self_part, "front", axis=0)
    upper_columns = gather_rows(upper_own, 1)
    upper_inverse = inverse_factor(upper_pivots[None], upper_columns)
    sums, mirror = fold(weights, turned_all)
    landed = mirror_blocks(mirror)
    upper_panel, upper_schur = parent_schur(
        parent_order, upper_pivots[None], weights, upper_own, upper_columns, upper_inverse,
        self_all, sums, landed, parent_fronts[0],
    )
    return (panel_rows[None], upper_panel[None], upper_schur[None])


def solution(mesh):
    in_specs = (P("front", "grid", None), P("front", "grid", None), P(), P(), P(), P())
    out_specs = (P("front", "grid", None), P("front", "grid", None), P("front", "grid", None))
    return jax.shard_map(
        on_device, mesh=mesh, in_specs=in_specs, out_specs=out_specs, check_vma=False
    )
```

```python
import functools

import jax
import jax.numpy as jnp
from jax import lax
from jax.experimental import pallas as pl
from jax.experimental.pallas import tpu as pltpu
from jax.sharding import PartitionSpec as P

PMAX = 256
CHIPS = 16
SIDE = 4
ROWS = 192
WIDE = 384
ORDER = 6144
BASE = 32
GROUP = 8
LEAD = 256
MESH = pl.DeviceIdType.MESH
SELF = ((0, 0), (0, 2), (2, 0), (2, 2))
TURNED = ((0, 1), (1, 0), (3, 3), (3, 1), (1, 2), (2, 3))
F32 = jnp.float32
BF16 = jnp.bfloat16
VMEM = pltpu.VMEM
NT = (((1,), (1,)), ((), ()))
NN = (((1,), (0,)), ((), ()))
TN = (((0,), (0,)), ((), ()))


def dot(a, b, dims):
    return lax.dot_general(a, b, dims, preferred_element_type=F32)


def split(a):
    high = a.astype(BF16)
    low = (a - high.astype(F32)).astype(BF16)
    return high, low


def product(a, b, dims):
    a_high, a_low = split(a)
    b_high, b_low = split(b)
    return dot(a_high, b_high, dims) + (dot(a_high, b_low, dims) + dot(a_low, b_high, dims))


def pick(one_hot, a, dims):
    a_high, a_low = split(a)
    return dot(one_hot, a_high, dims) + dot(one_hot, a_low, dims)


def exact(a, b, dims):
    return lax.dot_general(a, b, dims, precision=lax.Precision.HIGHEST, preferred_element_type=F32)


def shifted(chip, offset, sign=1):
    x = (chip // SIDE + sign * offset[0] + SIDE) % SIDE
    y = (chip % SIDE + sign * offset[1] + SIDE) % SIDE
    return x * SIDE + y


def remote(src, dst, sems, index, device):
    return pltpu.make_async_remote_copy(
        src_ref=src, dst_ref=dst, send_sem=sems[0].at[index], recv_sem=sems[1].at[index],
        device_id=device, device_id_type=MESH,
    )


def greet(devices, more=0):
    barrier = pltpu.get_barrier_semaphore()
    for device in devices:
        pl.semaphore_signal(barrier, inc=1, device_id=device, device_id_type=MESH)
    pl.semaphore_wait(barrier, len(devices) + more)


def cholesky_kernel(pivots_ref, block_ref, inverse_ref, work):
    rows = lax.broadcasted_iota(jnp.int32, (PMAX, PMAX), 0)
    columns = lax.broadcasted_iota(jnp.int32, (PMAX, PMAX), 1)
    same = (rows == columns).astype(F32)
    pivots = pivots_ref[0]
    work[:, :PMAX] = jnp.where((rows < pivots) & (columns < pivots), block_ref[...], same)
    work[:, PMAX:] = same
    small_rows = lax.broadcasted_iota(jnp.int32, (BASE, 1), 0)
    eye_rows = lax.broadcasted_iota(jnp.int32, (BASE, BASE), 0)
    eye_columns = lax.broadcasted_iota(jnp.int32, (BASE, BASE), 1)
    eye = (eye_rows == eye_columns).astype(F32)
    for step in range(PMAX // BASE):
        first = step * BASE
        last = first + BASE
        diagonal = work[first:last, first:last]
        both = jnp.concatenate([diagonal, eye, jnp.zeros((BASE, 128 - 2 * BASE), F32)], axis=1)
        for group in range(0, BASE, GROUP):
            columns_of = [jnp.broadcast_to(both[:, group + i : group + i + 1], (BASE, 128)) for i in range(GROUP)]
            rows_of = [both[group + i : group + i + 1, :] for i in range(GROUP)]
            for i in range(GROUP):
                k = group + i
                below = jnp.where(small_rows > k, columns_of[i], 0.0)
                inverse_pivot = 1.0 / columns_of[i][k : k + 1, :]
                scaled = rows_of[i] * inverse_pivot
                for j in range(i + 1, GROUP):
                    entry = columns_of[i][group + j : group + j + 1, :]
                    columns_of[j] = columns_of[j] - below * (entry * inverse_pivot)
                    rows_of[j] = rows_of[j] - entry * scaled
                both = both - below * scaled
        pivot_values = jnp.sum(both[:, :BASE] * eye, axis=1, keepdims=True)
        inverse = both[:, BASE : 2 * BASE] / jnp.sqrt(pivot_values)
        strip = exact(inverse, work[first:last, :], NN)
        work[first:last, :] = strip
        if last < PMAX:
            update = exact(strip[:, :PMAX], strip, TN)
            work[last:, :] = work[last:, :] - update[last:, :]
    inverse_ref[...] = jnp.where(rows < pivots, work[:, PMAX:], 0.0)


def inverse_factor(pivots, columns):
    return pl.pallas_call(
        cholesky_kernel,
        grid=(1,),
        out_shape=jax.ShapeDtypeStruct((PMAX, PMAX), F32),
        in_specs=[pl.BlockSpec(memory_space=pltpu.SMEM), pl.BlockSpec((PMAX, PMAX), lambda j: (0, 0))],
        out_specs=pl.BlockSpec((PMAX, PMAX), lambda j: (0, 0)),
        scratch_shapes=[pltpu.VMEM((PMAX, 2 * PMAX), F32)],
        cost_estimate=pl.CostEstimate(flops=400_000_000, bytes_accessed=524288, transcendentals=0),
        name="inverse_factor",
    )(pivots, columns)


def gather_stages(own_ref, all_ref, local_sem, send_sems, recv_sems, more=0):
    rank = lax.axis_index("grid")
    core = rank % 2
    chip = rank // 2
    x, y = chip // SIDE, chip % SIDE
    p = y + core * (x - y)
    s = x + core * (y - x)

    def device(dp, ds):
        pp, ss = (p + dp) % SIDE, (s + ds) % SIDE
        return 2 * (pp * (1 + 3 * core) + ss * (4 - 3 * core)) + core

    def rows(dp, ds, half=None):
        first = device(dp, ds) * ROWS
        if half is None:
            return pl.ds(pl.multiple_of(first, 64), ROWS)
        return pl.ds(pl.multiple_of(first + half * (ROWS // 2), 32), ROWS // 2)

    sems = (send_sems, recv_sems)
    sibling = {"grid": rank + 1 - 2 * core}
    p_up, p_down = {"grid": device(1, 0)}, {"grid": device(3, 0)}
    s_up, s_down = {"grid": device(0, 1)}, {"grid": device(0, 3)}
    greet((p_up, p_down, s_up, s_down, sibling), more)
    here = pltpu.make_async_copy(own_ref, all_ref.at[rows(0, 0)], local_sem)
    copies = []

    def send(index, where, target, source=None):
        copy = remote(all_ref.at[where] if source is None else source, all_ref.at[where], sems, index, target)
        copy.start()
        copies.append(copy)

    def arrived(index, where):
        remote(all_ref.at[where], all_ref.at[where], sems, index, sibling).wait_recv()

    def across(dp, ds, source=None):
        send(20 + 4 * dp + ds, rows(dp, ds), sibling, source)

    def sideways(dp):
        send(4 + dp, rows(dp, 0), s_up)
        send(8 + dp, rows(dp, 0), s_down)

    def begin():
        here.start()
        send(0, rows(0, 0), p_up, own_ref)
        send(1, rows(0, 0), p_down, own_ref)
        send(4, rows(0, 0), s_up, own_ref)
        send(8, rows(0, 0), s_down, own_ref)
        across(0, 0, own_ref)

    def from_below():
        arrived(0, rows(3, 0))
        send(2, rows(3, 0, 0), p_up)
        sideways(3)
        across(3, 0)

    def from_above():
        arrived(1, rows(1, 0))
        send(3, rows(1, 0, 1), p_down)
        sideways(1)
        across(1, 0)

    def pass_on(dp):
        arrived(4 + dp, rows(dp, 3))
        send(12 + dp, rows(dp, 3, 0), s_up)
        across(dp, 3)
        arrived(8 + dp, rows(dp, 1))
        send(16 + dp, rows(dp, 1, 1), s_down)
        across(dp, 1)

    def opposite():
        arrived(2, rows(2, 0, 0))
        arrived(3, rows(2, 0, 1))
        sideways(2)
        across(2, 0)

    def complete(dp):
        arrived(12 + dp, rows(dp, 2, 0))
        arrived(16 + dp, rows(dp, 2, 1))
        across(dp, 2)

    def finish():
        for copy in copies:
            copy.wait_send()
        for dp in range(SIDE):
            for ds in range(SIDE):
                chip_there = ((s + dp) % SIDE) * (4 - 3 * core) + ((p + ds) % SIDE) * (1 + 3 * core)
                first = (2 * chip_there + 1 - core) * ROWS
                arrived(20 + 4 * dp + ds, pl.ds(pl.multiple_of(first, 64), ROWS))
        here.wait()

    steps = [begin, from_below, from_above, functools.partial(pass_on, 0), opposite]
    steps += [functools.partial(pass_on, dp) for dp in (3, 1, 2)]
    steps += [functools.partial(complete, dp) for dp in (0, 3, 1, 2)]
    return steps + [finish]


def front_kernel(
    places_ref, rows_ref, own_ref, all_ref, turned_ref, both, local_sem, send_sems, recv_sems, own_sems, out_sems, in_sems
):
    rank = lax.axis_index("grid")
    core = rank % 2
    steps = gather_stages(own_ref, all_ref, local_sem, send_sems, recv_sems)
    sibling = {"grid": rank + 1 - 2 * core}
    mine = pl.ds(pl.multiple_of(core * ROWS, 64), ROWS)

    def local(j):
        lanes = pl.ds(pl.multiple_of(j * WIDE, 128), WIDE)
        return pltpu.make_async_copy(rows_ref.at[:, lanes], both.at[mine, lanes], own_sems.at[j])

    def pair(j):
        lanes = pl.ds(pl.multiple_of(j * WIDE, 128), WIDE)
        return pltpu.make_async_remote_copy(
            src_ref=rows_ref.at[:, lanes], dst_ref=both.at[mine, lanes],
            send_sem=out_sems.at[j], recv_sem=in_sems.at[j], device_id=sibling, device_id_type=MESH,
        )

    steps[0]()
    for j in range(CHIPS):
        pair(j).start()
        local(j).start()

    def here(j):
        local(j).wait()
        pair(j).wait()

    def work(j, carry):
        @pl.when(j < CHIPS - 1)
        def _():
            here(j + 1)

        first = j * WIDE + core * ROWS
        start = jnp.minimum(j * WIDE + core * 128, ORDER - 512)
        lanes = pl.ds(pl.multiple_of(start, 128), 512)
        wanted = first + lax.broadcasted_iota(jnp.int32, (ROWS, 512), 0)
        one_hot = (wanted == places_ref[:1, lanes]).astype(F32).astype(BF16)
        turned_ref[j] = pick(one_hot, both[:, lanes], NT)
        return carry

    here(0)
    done = 0
    rest = steps[1:-1]
    for index, step in enumerate(rest):
        until = (CHIPS * (index + 1)) // len(rest)
        lax.fori_loop(done, until, work, 0)
        done = until
        step()
    steps[-1]()


def front(rows, places):
    return pl.pallas_call(
        front_kernel,
        grid=(1,),
        out_shape=(
            jax.ShapeDtypeStruct((ORDER, PMAX), F32),
            jax.ShapeDtypeStruct((CHIPS, ROWS, WIDE), F32),
        ),
        in_specs=[
            pl.BlockSpec(places.shape, lambda i: (0, 0)),
            pl.BlockSpec(memory_space=pl.ANY),
            pl.BlockSpec((ROWS, PMAX), lambda i: (0, 0)),
        ],
        out_specs=(
            pl.BlockSpec((ORDER, PMAX), lambda i: (0, 0)),
            pl.BlockSpec((CHIPS, ROWS, WIDE), lambda i: (0, 0, 0)),
        ),
        scratch_shapes=[
            pltpu.VMEM((WIDE, ORDER), F32),
            pltpu.SemaphoreType.DMA,
            pltpu.SemaphoreType.DMA((36,)),
            pltpu.SemaphoreType.DMA((36,)),
            pltpu.SemaphoreType.DMA((CHIPS,)),
            pltpu.SemaphoreType.DMA((CHIPS,)),
            pltpu.SemaphoreType.DMA((CHIPS,)),
        ],
        compiler_params=pltpu.CompilerParams(collective_id=0, has_side_effects=True),
        cost_estimate=pl.CostEstimate(flops=400_000_000, bytes_accessed=25_000_000, transcendentals=0),
        name="front",
    )(places, rows, rows)


def offset_chip(chip, index, sign=1):
    dx, dy = 0, 0
    for number, (x, y) in enumerate(TURNED + SELF):
        dx = dx + jnp.where(index == number, x, 0)
        dy = dy + jnp.where(index == number, y, 0)
    return shifted(chip, (dx, dy), sign)


def post_kernel(
    weight_ref, places_ref, columns_ref, inverse_ref, moved_ref, front_ref,
    panel_ref, all_ref, sum_ref, landing_ref,
    blocks, lead, lead_landing, upper_own, z_landing, mirror, window, solved,
    local_sem, send_sems, recv_sems, z_send, z_recv, mirror_send, mirror_recv, lead_send, lead_recv,
):
    group = lax.axis_index("front")
    rank = lax.axis_index("grid")
    core = rank % 2
    chip = rank // 2
    turned = len(TURNED)
    total = turned + len(SELF)
    up, down = {"front": (group + 1) % SIDE}, {"front": (group + 3) % SIDE}
    others = [{"front": (group + d) % SIDE} for d in range(1, SIDE)]

    def mirror_device(index, k, sign):
        return {"grid": 2 * offset_chip(chip, index, sign) + k}

    barrier = pltpu.get_barrier_semaphore()
    for device in others:
        pl.semaphore_signal(barrier, inc=1, device_id=device, device_id_type=MESH)
    for index in range(turned):
        for k in range(2):
            pl.semaphore_signal(barrier, inc=1, device_id=mirror_device(index, k, -1), device_id_type=MESH)
    steps = gather_stages(upper_own, all_ref, local_sem, send_sems, recv_sems, len(others) + 2 * turned)

    inverse = inverse_ref[...]
    panel_ref[...] = exact(columns_ref[pl.ds(pl.multiple_of(rank * ROWS, 64), ROWS), :], inverse, NT)
    after = jnp.minimum(chip + 1, CHIPS - 1)

    def piece(index):
        return columns_ref[pl.ds(pl.multiple_of(index * WIDE, 128), WIDE), :]

    def places_at(index):
        return places_ref[:1, pl.ds(pl.multiple_of(index * WIDE, 128), WIDE)]

    wanted_rows = rank * ROWS + lax.broadcasted_iota(jnp.int32, (ROWS, WIDE), 0)
    picked = pick((wanted_rows == places_at(chip)).astype(F32).astype(BF16), piece(chip), NN)
    picked += pick((wanted_rows == places_at(chip + 1)).astype(F32).astype(BF16), piece(after), NN)
    solved[...] = exact(exact(picked, inverse, NT), inverse, NN)

    def block(where):
        following = jnp.minimum(where + 1, CHIPS - 1)
        w = solved[...]
        window[:, :WIDE] = moved_ref[where] - product(w, piece(where), NT)
        window[:, WIDE:] = moved_ref[following] - product(w, piece(following), NT)
        first = where * WIDE

        def part(low, wide):
            wanted = first + low + lax.broadcasted_iota(jnp.int32, (wide, wide + 256), 0)
            lanes = pl.ds(pl.multiple_of(first + low, 128), wide + 256)
            one_hot = (wanted == places_ref[:1, lanes]).astype(F32).astype(BF16)
            high, rest = split(window[:, low : low + wide + 256])
            return dot(high, one_hot, NT) + dot(rest, one_hot, NT)

        return jnp.concatenate([part(0, 256), part(256, 128)], axis=1)

    z_sems = (z_send, z_recv)
    upper, lower = pl.ds(0, ROWS // 2), pl.ds(ROWS // 2, ROWS // 2)

    def z_copy(index, which):
        if which == 0:
            return remote(blocks.at[index], z_landing.at[0, index], z_sems, 4 * index, up)
        if which == 1:
            return remote(blocks.at[index], z_landing.at[2, index], z_sems, 4 * index + 1, down)
        if which == 2:
            return remote(z_landing.at[0, index, upper], z_landing.at[1, index, upper], z_sems, 4 * index + 2, up)
        return remote(z_landing.at[2, index, lower], z_landing.at[1, index, lower], z_sems, 4 * index + 3, down)

    def z_begin(index):
        z_copy(index, 0).start()
        z_copy(index, 1).start()

    def z_forward(index):
        z_copy(index, 0).wait_recv()
        z_copy(index, 2).start()
        z_copy(index, 1).wait_recv()
        z_copy(index, 3).start()

    def z_sum(index):
        z_copy(index, 2).wait_recv()
        z_copy(index, 3).wait_recv()
        result = weight_ref[0] * blocks[index]
        for d in range(SIDE - 1):
            result = result + weight_ref[d + 1] * z_landing[d, index]
        sum_ref[index] = result
        return result

    def lead_copy(d):
        return remote(lead.at[:, pl.ds(0, LEAD)], lead_landing.at[d], (lead_send, lead_recv), d, others[d])

    def mirror_copy(index, k, arriving=False):
        slot = k if arriving else core
        return pltpu.make_async_remote_copy(
            src_ref=mirror.at[index, k], dst_ref=landing_ref.at[index, slot],
            send_sem=mirror_send.at[2 * index + k], recv_sem=mirror_recv.at[2 * index + slot],
            device_id=mirror_device(index, k, 1), device_id_type=MESH,
        )

    def fold(index, carry):
        turned_block = z_sum(index).T

        @pl.when(index > 0)
        def _():
            for k in range(2):
                mirror_copy(index - 1, k).start()

        mirror[index, 0] = turned_block[:ROWS]
        mirror[index, 1] = turned_block[ROWS:]
        return carry

    lead[...] = block(0 * chip)

    def compute(index, carry):
        result = block(offset_chip(chip, index))

        @pl.when(index == 0)
        def _():
            for d in range(SIDE - 1):
                lead_copy(d).start()

        @pl.when((index > 0) & (index <= turned))
        def _():
            z_begin(index - 1)

        blocks[index] = result
        return carry

    lax.fori_loop(0, total, compute, 0)
    leading = front_ref[...] + weight_ref[0] * lead[:, :LEAD]
    for d in range(SIDE - 1):
        lead_copy(d).wait()
        leading = leading + weight_ref[d + 1] * lead_landing[d]
    upper_own[...] = leading
    z_forward(0)
    steps[0]()
    z_forward(1)
    steps[1]()
    steps[2]()
    z_forward(2)
    steps[3]()
    steps[4]()
    z_forward(3)
    steps[5]()
    steps[6]()
    z_forward(4)
    steps[7]()
    z_forward(5)

    def z_rest(index, carry):
        z_begin(index)
        return carry

    lax.fori_loop(turned, total, z_rest, 0)
    for step in steps[8:]:
        step()
    lax.fori_loop(0, turned, fold, 0)

    def forward(index, carry):
        z_forward(index)
        return carry

    lax.fori_loop(turned, turned + 1, forward, 0)
    for k in range(2):
        mirror_copy(turned - 1, k).start()
    lax.fori_loop(turned + 1, total, forward, 0)

    def own_sum(index, carry):
        z_sum(index)
        return carry

    lax.fori_loop(turned, total, own_sum, 0)

    def drain(index, carry):
        for which in range(4):
            z_copy(index, which).wait_send()
        return carry

    lax.fori_loop(0, total, drain, 0)

    def settle(index, carry):
        for k in range(2):
            mirror_copy(index, k).wait_send()
            mirror_copy(index, k, True).wait_recv()
        return carry

    lax.fori_loop(0, turned, settle, 0)


def post(weights, places, columns, inverse, moved, front):
    turned = len(TURNED)
    total = turned + len(SELF)
    dma = pltpu.SemaphoreType.DMA
    whole = lambda shape: pl.BlockSpec(shape, lambda i: (0,) * len(shape))
    outs = [(ROWS, PMAX), (ORDER, PMAX), (total, ROWS, WIDE), (turned, 2, ROWS, ROWS)]
    return pl.pallas_call(
        post_kernel,
        grid=(1,),
        out_shape=tuple(jax.ShapeDtypeStruct(shape, F32) for shape in outs),
        in_specs=[
            pl.BlockSpec(memory_space=pltpu.SMEM),
            whole(places.shape),
            whole((ORDER, PMAX)),
            whole((PMAX, PMAX)),
            whole((CHIPS, ROWS, WIDE)),
            pl.BlockSpec((ROWS, LEAD), lambda i: (0, 0)),
        ],
        out_specs=tuple(whole(shape) for shape in outs),
        scratch_shapes=[
            pltpu.VMEM((total, ROWS, WIDE), F32),
            pltpu.VMEM((ROWS, WIDE), F32),
            pltpu.VMEM((SIDE - 1, ROWS, LEAD), F32),
            pltpu.VMEM((ROWS, LEAD), F32),
            pltpu.VMEM((SIDE - 1, total, ROWS, WIDE), F32),
            pltpu.VMEM((turned, 2, ROWS, ROWS), F32),
            pltpu.VMEM((ROWS, 2 * WIDE), F32),
            pltpu.VMEM((ROWS, PMAX), F32),
            dma,
            dma((36,)),
            dma((36,)),
            dma((4 * total,)),
            dma((4 * total,)),
            dma((2 * turned,)),
            dma((2 * turned,)),
            dma((SIDE - 1,)),
            dma((SIDE - 1,)),
        ],
        compiler_params=pltpu.CompilerParams(collective_id=1, has_side_effects=True),
        cost_estimate=pl.CostEstimate(flops=400_000_000, bytes_accessed=25_000_000, transcendentals=0),
        name="post",
    )(weights, places, columns, inverse, moved, front)


def parent_kernel(
    order_ref, pivots_ref, own_ref, here_ref, inverse_ref, sum_ref, mirror_ref, front_ref, panel_ref, schur_ref, weights
):
    step = pl.program_id(0)
    grid_rank = lax.axis_index("grid")
    sums = len(TURNED) + len(SELF)

    @pl.when(step == 0)
    def _():
        inverse = inverse_ref[...]
        panel = exact(own_ref[...], inverse, NT)
        panel_ref[...] = panel
        weights[...] = exact(panel, inverse, NN)

    total = front_ref[...] - product(here_ref[...], weights[...], NT).T
    pivots = pivots_ref[0]
    rows = grid_rank * ROWS + lax.broadcasted_iota(jnp.int32, (ROWS, WIDE), 0)
    columns = order_ref[step] * WIDE + lax.broadcasted_iota(jnp.int32, (ROWS, WIDE), 1)
    keep = (rows >= pivots) & (columns >= pivots)

    @pl.when(step < sums)
    def _():
        schur_ref[...] = jnp.where(keep, total + sum_ref[0], 0.0)

    @pl.when(step >= sums)
    def _():
        mirror = jnp.concatenate([mirror_ref[0, 0], mirror_ref[0, 1]], axis=1)
        schur_ref[...] = jnp.where(keep, total + mirror, 0.0)


def parent_schur(order, pivots, columns, inverse, sums, mirror, front):
    count = len(TURNED) + len(SELF)
    spec = pltpu.PrefetchScalarGridSpec(
        num_scalar_prefetch=1,
        grid=(CHIPS,),
        in_specs=[
            pl.BlockSpec(memory_space=pltpu.SMEM),
            pl.BlockSpec((ROWS, PMAX), lambda i, order: (order[CHIPS], 0)),
            pl.BlockSpec((WIDE, PMAX), lambda i, order: (order[i], 0)),
            pl.BlockSpec((PMAX, PMAX), lambda i, order: (0, 0)),
            pl.BlockSpec((1, ROWS, WIDE), lambda i, order: (jnp.minimum(i, count - 1), 0, 0)),
            pl.BlockSpec((1, 2, ROWS, ROWS), lambda i, order: (jnp.maximum(i - count, 0), 0, 0, 0)),
            pl.BlockSpec((ROWS, WIDE), lambda i, order: (0, order[i])),
        ],
        out_specs=(
            pl.BlockSpec((ROWS, PMAX), lambda i, order: (0, 0)),
            pl.BlockSpec((ROWS, WIDE), lambda i, order: (0, order[i])),
        ),
        scratch_shapes=[pltpu.VMEM((ROWS, PMAX), F32)],
    )
    return pl.pallas_call(
        parent_kernel,
        grid_spec=spec,
        out_shape=(jax.ShapeDtypeStruct((ROWS, PMAX), F32), jax.ShapeDtypeStruct((ROWS, ORDER), F32)),
        cost_estimate=pl.CostEstimate(flops=400_000_000, bytes_accessed=30_000_000, transcendentals=0),
        name="parent_schur",
    )(order, pivots, columns, columns, inverse, sums, mirror, front)


def on_device(child_fronts, parent_fronts, child_maps, parent_of, child_pivots, parent_pivots):
    front_group = lax.axis_index("front")
    rank = lax.axis_index("grid")
    chip = rank // 2
    front_rows = child_fronts[0]
    pivots = lax.dynamic_slice(child_pivots, (front_group,), (1,))
    upper_pivots = lax.dynamic_slice(parent_pivots, (front_group,), (1,))
    groups = (front_group - jnp.arange(SIDE, dtype=jnp.int32)) % SIDE
    weights = (parent_of[groups] == front_group).astype(F32)
    number = jnp.arange(CHIPS + 1, dtype=jnp.int32)
    count = len(TURNED) + len(SELF)
    sign = jnp.where(number < count, 1, -1)
    order = offset_chip(chip, jnp.where(number < count, number, number - count), sign)
    order = jnp.where(number < CHIPS, order, rank)

    position = jnp.arange(ORDER, dtype=jnp.int32)
    line = jnp.where(position >= pivots, child_maps[front_group], -1)
    line = jnp.pad(line, (0, 2 * WIDE), constant_values=-1)
    places = jnp.broadcast_to(line[None], (8, line.shape[0]))
    columns, turned = front(front_rows, places)
    same_core = [[2 * c + k for c in range(CHIPS)] for k in range(2)]
    moved = lax.all_to_all(turned, "grid", 0, 0, axis_index_groups=same_core)
    inverse = inverse_factor(pivots, columns)
    panel_rows, upper_columns, sums, mirror = post(weights, places, columns, inverse, moved, parent_fronts[0])
    upper_inverse = inverse_factor(upper_pivots, upper_columns)
    upper_panel, upper_schur = parent_schur(
        order, upper_pivots, upper_columns, upper_inverse, sums, mirror, parent_fronts[0]
    )
    return (panel_rows[None], upper_panel[None], upper_schur[None])


def solution(mesh):
    in_specs = (P("front", "grid", None), P("front", "grid", None), P(), P(), P(), P())
    out_specs = (P("front", "grid", None), P("front", "grid", None), P("front", "grid", None))
    return jax.shard_map(
        on_device, mesh=mesh, in_specs=in_specs, out_specs=out_specs, check_vma=False
    )
```

```python
import functools

import jax
import jax.numpy as jnp
from jax import lax
from jax.experimental import pallas as pl
from jax.experimental.pallas import tpu as pltpu
from jax.sharding import PartitionSpec as P

PMAX = 256
CHIPS = 16
SIDE = 4
ROWS = 192
WIDE = 384
ORDER = 6144
HALF = 96
BASE = 32
GROUP = 8
LEAD = 256
MESH = pl.DeviceIdType.MESH
SELF = ((0, 0), (0, 2), (2, 0), (2, 2))
TURNED = ((0, 1), (1, 0), (3, 3), (3, 1), (1, 2), (2, 3))
F32 = jnp.float32
BF16 = jnp.bfloat16
VMEM = pltpu.VMEM
NT = (((1,), (1,)), ((), ()))
NN = (((1,), (0,)), ((), ()))
TN = (((0,), (0,)), ((), ()))


def dot(a, b, dims):
    return lax.dot_general(a, b, dims, preferred_element_type=F32)


def split(a):
    high = a.astype(BF16)
    low = (a - high.astype(F32)).astype(BF16)
    return high, low


def product(a, b, dims):
    a_high, a_low = split(a)
    b_high, b_low = split(b)
    both = dot(jnp.concatenate([a_high, a_low], axis=0), b_high, dims)
    return both[: a.shape[0]] + (both[a.shape[0] :] + dot(a_high, b_low, dims))


def pick(one_hot, a, dims):
    a_high, a_low = split(a)
    return dot(one_hot, a_high, dims) + dot(one_hot, a_low, dims)


def exact(a, b, dims):
    return lax.dot_general(a, b, dims, precision=lax.Precision.HIGHEST, preferred_element_type=F32)


def shifted(chip, offset, sign=1):
    x = (chip // SIDE + sign * offset[0] + SIDE) % SIDE
    y = (chip % SIDE + sign * offset[1] + SIDE) % SIDE
    return x * SIDE + y


def remote(src, dst, sems, index, device):
    return pltpu.make_async_remote_copy(
        src_ref=src, dst_ref=dst, send_sem=sems[0].at[index], recv_sem=sems[1].at[index],
        device_id=device, device_id_type=MESH,
    )


def greet(devices, more=0):
    barrier = pltpu.get_barrier_semaphore()
    for device in devices:
        pl.semaphore_signal(barrier, inc=1, device_id=device, device_id_type=MESH)
    pl.semaphore_wait(barrier, len(devices) + more)


def factor_into(pivots, block, inverse_ref, work):
    rows = lax.broadcasted_iota(jnp.int32, (PMAX, PMAX), 0)
    columns = lax.broadcasted_iota(jnp.int32, (PMAX, PMAX), 1)
    same = (rows == columns).astype(F32)
    work[:, :PMAX] = jnp.where((rows < pivots) & (columns < pivots), block, same)
    work[:, PMAX:] = same
    small_rows = lax.broadcasted_iota(jnp.int32, (BASE, 1), 0)
    eye_rows = lax.broadcasted_iota(jnp.int32, (BASE, 128), 0)
    eye_columns = lax.broadcasted_iota(jnp.int32, (BASE, 128), 1)
    eye = (eye_rows == eye_columns).astype(F32)
    eye_after = (eye_rows + BASE == eye_columns).astype(F32)
    all_rows = lax.broadcasted_iota(jnp.int32, (PMAX, 1), 0)
    tall_rows = lax.broadcasted_iota(jnp.int32, (PMAX, 128), 0)
    tall_columns = lax.broadcasted_iota(jnp.int32, (PMAX, 128), 1)

    def step(index, carry):
        first = index * BASE
        here = pl.ds(pl.multiple_of(first, BASE), BASE)
        chosen = ((tall_rows == tall_columns + first) & (tall_columns < BASE)).astype(F32)
        both = exact(work[here, :PMAX], chosen, NN) + eye_after
        for group in range(0, BASE, GROUP):
            columns_of = [jnp.broadcast_to(both[:, group + i : group + i + 1], (BASE, 128)) for i in range(GROUP)]
            rows_of = [both[group + i : group + i + 1, :] for i in range(GROUP)]
            for i in range(GROUP):
                k = group + i
                below = jnp.where(small_rows > k, columns_of[i], 0.0)
                inverse_pivot = 1.0 / columns_of[i][k : k + 1, :]
                scaled = rows_of[i] * inverse_pivot
                for j in range(i + 1, GROUP):
                    entry = columns_of[i][group + j : group + j + 1, :]
                    columns_of[j] = columns_of[j] - below * (entry * inverse_pivot)
                    rows_of[j] = rows_of[j] - entry * scaled
                both = both - below * scaled
        pivot_values = jnp.sum(both * eye, axis=1, keepdims=True)
        inverse = both[:, BASE : 2 * BASE] / jnp.sqrt(pivot_values)
        strip = exact(inverse, work[here, :], NN)
        update = exact(strip[:, :PMAX], strip, TN)
        work[...] = work[...] - jnp.where(all_rows >= first + BASE, update, 0.0)
        work[here, :] = strip
        return carry

    lax.fori_loop(0, PMAX // BASE, step, 0)
    inverse_ref[...] = jnp.where(rows < pivots, work[:, PMAX:], 0.0)


def cholesky_kernel(pivots_ref, block_ref, inverse_ref, work):
    factor_into(pivots_ref[0], block_ref[...], inverse_ref, work)


def inverse_factor(pivots, columns):
    return pl.pallas_call(
        cholesky_kernel,
        grid=(1,),
        out_shape=jax.ShapeDtypeStruct((PMAX, PMAX), F32),
        in_specs=[pl.BlockSpec(memory_space=pltpu.SMEM), pl.BlockSpec((PMAX, PMAX), lambda j: (0, 0))],
        out_specs=pl.BlockSpec((PMAX, PMAX), lambda j: (0, 0)),
        scratch_shapes=[pltpu.VMEM((PMAX, 2 * PMAX), F32)],
        cost_estimate=pl.CostEstimate(flops=400_000_000, bytes_accessed=524288, transcendentals=0),
        name="inverse_factor",
    )(pivots, columns)


def gather_stages(own_ref, all_ref, local_sem, send_sems, recv_sems, more=0):
    rank = lax.axis_index("grid")
    core = rank % 2
    chip = rank // 2
    x, y = chip // SIDE, chip % SIDE
    p = y + core * (x - y)
    s = x + core * (y - x)

    def device(dp, ds):
        pp, ss = (p + dp) % SIDE, (s + ds) % SIDE
        return 2 * (pp * (1 + 3 * core) + ss * (4 - 3 * core)) + core

    def rows(dp, ds, half=None):
        first = device(dp, ds) * ROWS
        if half is None:
            return pl.ds(pl.multiple_of(first, 64), ROWS)
        return pl.ds(pl.multiple_of(first + half * (ROWS // 2), 32), ROWS // 2)

    sems = (send_sems, recv_sems)
    sibling = {"grid": rank + 1 - 2 * core}
    p_up, p_down = {"grid": device(1, 0)}, {"grid": device(3, 0)}
    s_up, s_down = {"grid": device(0, 1)}, {"grid": device(0, 3)}
    greet((p_up, p_down, s_up, s_down, sibling), more)
    here = pltpu.make_async_copy(own_ref, all_ref.at[rows(0, 0)], local_sem)
    copies = []

    def send(index, where, target, source=None):
        copy = remote(all_ref.at[where] if source is None else source, all_ref.at[where], sems, index, target)
        copy.start()
        copies.append(copy)

    def arrived(index, where):
        remote(all_ref.at[where], all_ref.at[where], sems, index, sibling).wait_recv()

    def across(dp, ds, source=None):
        send(20 + 4 * dp + ds, rows(dp, ds), sibling, source)

    def sideways(dp):
        send(4 + dp, rows(dp, 0), s_up)
        send(8 + dp, rows(dp, 0), s_down)

    def begin():
        here.start()
        send(0, rows(0, 0), p_up, own_ref)
        send(1, rows(0, 0), p_down, own_ref)
        send(4, rows(0, 0), s_up, own_ref)
        send(8, rows(0, 0), s_down, own_ref)
        across(0, 0, own_ref)

    def from_below():
        arrived(0, rows(3, 0))
        send(2, rows(3, 0, 0), p_up)
        sideways(3)
        across(3, 0)

    def from_above():
        arrived(1, rows(1, 0))
        send(3, rows(1, 0, 1), p_down)
        sideways(1)
        across(1, 0)

    def pass_on(dp):
        arrived(4 + dp, rows(dp, 3))
        send(12 + dp, rows(dp, 3, 0), s_up)
        across(dp, 3)
        arrived(8 + dp, rows(dp, 1))
        send(16 + dp, rows(dp, 1, 1), s_down)
        across(dp, 1)

    def opposite():
        arrived(2, rows(2, 0, 0))
        arrived(3, rows(2, 0, 1))
        sideways(2)
        across(2, 0)

    def complete(dp):
        arrived(12 + dp, rows(dp, 2, 0))
        arrived(16 + dp, rows(dp, 2, 1))
        across(dp, 2)

    def finish():
        for copy in copies:
            copy.wait_send()
        for dp in range(SIDE):
            for ds in range(SIDE):
                chip_there = ((s + dp) % SIDE) * (4 - 3 * core) + ((p + ds) % SIDE) * (1 + 3 * core)
                first = (2 * chip_there + 1 - core) * ROWS
                arrived(20 + 4 * dp + ds, pl.ds(pl.multiple_of(first, 64), ROWS))
        here.wait()

    steps = [begin, from_below, from_above, functools.partial(pass_on, 0), opposite]
    steps += [functools.partial(pass_on, dp) for dp in (3, 1, 2)]
    steps += [functools.partial(complete, dp) for dp in (0, 3, 1, 2)]
    return steps + [finish]


def front_kernel(
    places_ref, rows_ref, own_ref, all_ref, turned_ref, later_ref, both, local_sem, send_sems, recv_sems, own_sems, out_sems, in_sems
):
    rank = lax.axis_index("grid")
    core = rank % 2
    steps = gather_stages(own_ref, all_ref, local_sem, send_sems, recv_sems)
    sibling = {"grid": rank + 1 - 2 * core}
    mine = pl.ds(pl.multiple_of(core * ROWS, 64), ROWS)

    def local(j):
        lanes = pl.ds(pl.multiple_of(j * WIDE, 128), WIDE)
        return pltpu.make_async_copy(rows_ref.at[:, lanes], both.at[mine, lanes], own_sems.at[j])

    def pair(j):
        lanes = pl.ds(pl.multiple_of(j * WIDE, 128), WIDE)
        return pltpu.make_async_remote_copy(
            src_ref=rows_ref.at[:, lanes], dst_ref=both.at[mine, lanes],
            send_sem=out_sems.at[j], recv_sem=in_sems.at[j], device_id=sibling, device_id_type=MESH,
        )

    steps[0]()
    for j in range(CHIPS):
        pair(j).start()
        local(j).start()

    def here(j):
        local(j).wait()
        pair(j).wait()

    def work(j, carry):
        @pl.when(j < CHIPS - 1)
        def _():
            here(j + 1)

        first = j * WIDE + core * ROWS
        start = jnp.minimum(j * WIDE + core * 128, ORDER - 512)
        lanes = pl.ds(pl.multiple_of(start, 128), 512)
        wanted = first + lax.broadcasted_iota(jnp.int32, (ROWS, 512), 0)
        one_hot = (wanted == places_ref[:1, lanes]).astype(F32).astype(BF16)
        result = pick(one_hot, both[:, lanes], NT)
        turned_ref[j] = result[:HALF]
        later_ref[j] = result[HALF:]
        return carry

    here(0)
    done = 0
    rest = steps[1:-1]
    for index, step in enumerate(rest):
        until = (CHIPS * (index + 1)) // len(rest)
        lax.fori_loop(done, until, work, 0)
        done = until
        step()
    steps[-1]()


def front(rows, places):
    return pl.pallas_call(
        front_kernel,
        grid=(1,),
        out_shape=(
            jax.ShapeDtypeStruct((ORDER, PMAX), F32),
            jax.ShapeDtypeStruct((CHIPS, HALF, WIDE), F32),
            jax.ShapeDtypeStruct((CHIPS, HALF, WIDE), F32),
        ),
        in_specs=[
            pl.BlockSpec(places.shape, lambda i: (0, 0)),
            pl.BlockSpec(memory_space=pl.ANY),
            pl.BlockSpec((ROWS, PMAX), lambda i: (0, 0)),
        ],
        out_specs=(
            pl.BlockSpec((ORDER, PMAX), lambda i: (0, 0)),
            pl.BlockSpec((CHIPS, HALF, WIDE), lambda i: (0, 0, 0)),
            pl.BlockSpec((CHIPS, HALF, WIDE), lambda i: (0, 0, 0)),
        ),
        scratch_shapes=[
            pltpu.VMEM((WIDE, ORDER), F32),
            pltpu.SemaphoreType.DMA,
            pltpu.SemaphoreType.DMA((36,)),
            pltpu.SemaphoreType.DMA((36,)),
            pltpu.SemaphoreType.DMA((CHIPS,)),
            pltpu.SemaphoreType.DMA((CHIPS,)),
            pltpu.SemaphoreType.DMA((CHIPS,)),
        ],
        compiler_params=pltpu.CompilerParams(collective_id=0, has_side_effects=True),
        cost_estimate=pl.CostEstimate(flops=400_000_000, bytes_accessed=25_000_000, transcendentals=0),
        name="front",
    )(places, rows, rows)


def offset_chip(chip, index, sign=1):
    dx, dy = 0, 0
    for number, (x, y) in enumerate(TURNED + SELF):
        dx = dx + jnp.where(index == number, x, 0)
        dy = dy + jnp.where(index == number, y, 0)
    return shifted(chip, (dx, dy), sign)


LEAVING = (
    (0, 1), (1, 0), (0, 3), (3, 0), (1, 1), (3, 3), (1, 3), (3, 1),
    (0, 2), (2, 0), (1, 2), (2, 1), (3, 2), (2, 3), (2, 2),
)


def post_kernel(
    weight_ref, pivots_ref, places_ref, columns_ref, inverse_ref, moved_ref, later_ref, front_ref,
    panel_ref, all_ref, upper_inverse_ref, sum_ref, landing_ref,
    moved_later, blocks, lead, lead_landing, upper_own, z_landing, mirror, window, solved, work,
    local_sem, send_sems, recv_sems, z_send, z_recv, mirror_send, mirror_recv, lead_send, lead_recv,
    later_send, later_recv, later_local,
):
    group = lax.axis_index("front")
    rank = lax.axis_index("grid")
    core = rank % 2
    chip = rank // 2
    turned = len(TURNED)
    total = turned + len(SELF)
    up, down = {"front": (group + 1) % SIDE}, {"front": (group + 3) % SIDE}
    others = [{"front": (group + d) % SIDE} for d in range(1, SIDE)]

    def mirror_device(index, k, sign):
        return {"grid": 2 * offset_chip(chip, index, sign) + k}

    barrier = pltpu.get_barrier_semaphore()
    for device in others:
        pl.semaphore_signal(barrier, inc=1, device_id=device, device_id_type=MESH)
    for index in range(turned):
        for k in range(2):
            pl.semaphore_signal(barrier, inc=1, device_id=mirror_device(index, k, -1), device_id_type=MESH)
    for offset in LEAVING:
        device = {"grid": 2 * shifted(chip, offset) + core}
        pl.semaphore_signal(barrier, inc=1, device_id=device, device_id_type=MESH)
    more = len(others) + 2 * turned + len(LEAVING)
    steps = gather_stages(upper_own, all_ref, local_sem, send_sems, recv_sems, more)

    kept = pltpu.make_async_copy(later_ref.at[chip], moved_later.at[chip], later_local)
    kept.start()
    leaving = []
    for number, offset in enumerate(LEAVING):
        to = shifted(chip, offset, -1)
        copy = remote(
            later_ref.at[to], moved_later.at[chip], (later_send, later_recv), number, {"grid": 2 * to + core}
        )
        copy.start()
        leaving.append(copy)

    inverse = inverse_ref[...]
    panel_ref[...] = exact(columns_ref[pl.ds(pl.multiple_of(rank * ROWS, 64), ROWS), :], inverse, NT)
    after = jnp.minimum(chip + 1, CHIPS - 1)

    def piece(index):
        return columns_ref[pl.ds(pl.multiple_of(index * WIDE, 128), WIDE), :]

    def places_at(index):
        return places_ref[:1, pl.ds(pl.multiple_of(index * WIDE, 128), WIDE)]

    wanted_rows = rank * ROWS + lax.broadcasted_iota(jnp.int32, (ROWS, WIDE), 0)
    picked = pick((wanted_rows == places_at(chip)).astype(F32).astype(BF16), piece(chip), NN)
    picked += pick((wanted_rows == places_at(chip + 1)).astype(F32).astype(BF16), piece(after), NN)
    solved[...] = exact(exact(picked, inverse, NT), inverse, NN)

    def block(where, half):
        source = moved_later if half else moved_ref
        following = jnp.minimum(where + 1, CHIPS - 1)
        w = solved[half * HALF : (half + 1) * HALF, :]
        window[:, :WIDE] = source[where] - product(piece(where), w, NT).T
        window[:, WIDE:] = source[following] - product(piece(following), w, NT).T
        first = where * WIDE

        def part(low, wide):
            wanted = first + low + lax.broadcasted_iota(jnp.int32, (wide, wide + 256), 0)
            lanes = pl.ds(pl.multiple_of(first + low, 128), wide + 256)
            one_hot = (wanted == places_ref[:1, lanes]).astype(F32).astype(BF16)
            both = dot(jnp.concatenate(split(window[:, low : low + wide + 256]), axis=0), one_hot, NT)
            return both[:HALF] + both[HALF:]

        return jnp.concatenate([part(0, 256), part(256, 128)], axis=1)

    z_sems = (z_send, z_recv)

    def z_copy(index, half, which):
        sem = 4 * (2 * index + half) + which
        every = pl.ds(half * HALF, HALF)
        upper = pl.ds(half * HALF, HALF // 2)
        lower = pl.ds(half * HALF + HALF // 2, HALF // 2)
        if which == 0:
            return remote(blocks.at[index, every], z_landing.at[0, index, every], z_sems, sem, up)
        if which == 1:
            return remote(blocks.at[index, every], z_landing.at[2, index, every], z_sems, sem, down)
        if which == 2:
            return remote(z_landing.at[0, index, upper], z_landing.at[1, index, upper], z_sems, sem, up)
        return remote(z_landing.at[2, index, lower], z_landing.at[1, index, lower], z_sems, sem, down)

    def z_begin(index, half):
        z_copy(index, half, 0).start()
        z_copy(index, half, 1).start()

    def z_forward(index, half):
        z_copy(index, half, 0).wait_recv()
        z_copy(index, half, 2).start()
        z_copy(index, half, 1).wait_recv()
        z_copy(index, half, 3).start()

    def z_sum(index, half):
        z_copy(index, half, 2).wait_recv()
        z_copy(index, half, 3).wait_recv()
        every = pl.ds(half * HALF, HALF)
        result = weight_ref[0] * blocks[index, every]
        for d in range(SIDE - 1):
            result = result + weight_ref[d + 1] * z_landing[d, index, every]
        sum_ref[index, every] = result
        return result

    def lead_copy(d):
        return remote(lead.at[:, pl.ds(0, LEAD)], lead_landing.at[d], (lead_send, lead_recv), d, others[d])

    def mirror_copy(index, half, k, arriving=False):
        slot = k if arriving else core
        return pltpu.make_async_remote_copy(
            src_ref=mirror.at[index, half, k], dst_ref=landing_ref.at[index, slot, half],
            send_sem=mirror_send.at[4 * index + 2 * half + k],
            recv_sem=mirror_recv.at[4 * index + 2 * half + slot],
            device_id=mirror_device(index, k, 1), device_id_type=MESH,
        )

    def mirror_begin(index, half):
        for k in range(2):
            mirror_copy(index, half, k).start()

    def each(first, last, work):
        def body(index, carry):
            work(index)
            return carry

        lax.fori_loop(first, last, body, 0)

    def fold(half):
        def work(index):
            turned_block = z_sum(index, half).T

            @pl.when(index > 0)
            def _():
                mirror_begin(index - 1, half)

            mirror[index, half, 0] = turned_block[:ROWS]
            mirror[index, half, 1] = turned_block[ROWS:]

        return work

    def compute(half):
        def work(index):
            result = block(offset_chip(chip, index), half)

            @pl.when((index > 0) & (index <= turned))
            def _():
                z_begin(index - 1, half)

            blocks[index, half * HALF : (half + 1) * HALF] = result

        return work

    lead[:HALF] = block(0 * chip, 0)
    each(0, total, compute(0))
    each(0, turned, lambda index: z_forward(index, 0))
    each(turned, total, lambda index: z_begin(index, 0))
    each(0, turned, fold(0))
    for copy in leaving:
        copy.wait()
    kept.wait()
    lead[HALF:] = block(0 * chip, 1)
    mirror_begin(turned - 1, 0)
    each(0, 1, compute(1))
    for d in range(SIDE - 1):
        lead_copy(d).start()
    each(1, turned + 1, compute(1))
    each(turned, total, lambda index: z_forward(index, 0))
    each(turned + 1, total, compute(1))
    leading = front_ref[...] + weight_ref[0] * lead[:, :LEAD]
    for d in range(SIDE - 1):
        lead_copy(d).wait()
        leading = leading + weight_ref[d + 1] * lead_landing[d]
    upper_own[...] = leading
    z_forward(0, 1)
    steps[0]()
    z_forward(1, 1)
    steps[1]()
    steps[2]()
    z_forward(2, 1)
    steps[3]()
    z_begin(turned, 1)
    z_forward(3, 1)
    steps[4]()
    steps[5]()
    z_forward(4, 1)
    z_begin(turned + 1, 1)
    steps[6]()
    z_forward(5, 1)
    each(turned + 2, total, lambda index: z_begin(index, 1))
    for step in steps[7:]:
        step()
    each(0, turned, fold(1))
    each(turned, turned + 2, lambda index: z_forward(index, 1))
    mirror_begin(turned - 1, 1)
    factor_into(pivots_ref[0], all_ref[:PMAX, :], upper_inverse_ref, work)
    each(turned + 2, total, lambda index: z_forward(index, 1))
    each(turned, total, lambda index: z_sum(index, 0))
    each(turned, total, lambda index: z_sum(index, 1))

    def drain(index):
        for half in range(2):
            for which in range(4):
                z_copy(index, half, which).wait_send()

    def settle(index):
        for half in range(2):
            for k in range(2):
                mirror_copy(index, half, k).wait_send()
                mirror_copy(index, half, k, True).wait_recv()

    each(0, total, drain)
    each(0, turned, settle)


def post(weights, pivots, places, columns, inverse, moved, later, front):
    turned = len(TURNED)
    total = turned + len(SELF)
    dma = pltpu.SemaphoreType.DMA
    whole = lambda shape: pl.BlockSpec(shape, lambda i: (0,) * len(shape))
    outs = [(ROWS, PMAX), (ORDER, PMAX), (PMAX, PMAX), (total, ROWS, WIDE), (turned, 2, 2, ROWS, HALF)]
    return pl.pallas_call(
        post_kernel,
        grid=(1,),
        out_shape=tuple(jax.ShapeDtypeStruct(shape, F32) for shape in outs),
        in_specs=[
            pl.BlockSpec(memory_space=pltpu.SMEM),
            pl.BlockSpec(memory_space=pltpu.SMEM),
            whole(places.shape),
            whole((ORDER, PMAX)),
            whole((PMAX, PMAX)),
            whole((CHIPS, HALF, WIDE)),
            whole((CHIPS, HALF, WIDE)),
            pl.BlockSpec((ROWS, LEAD), lambda i: (0, 0)),
        ],
        out_specs=tuple(whole(shape) for shape in outs),
        scratch_shapes=[
            pltpu.VMEM((CHIPS, HALF, WIDE), F32),
            pltpu.VMEM((total, ROWS, WIDE), F32),
            pltpu.VMEM((ROWS, WIDE), F32),
            pltpu.VMEM((SIDE - 1, ROWS, LEAD), F32),
            pltpu.VMEM((ROWS, LEAD), F32),
            pltpu.VMEM((SIDE - 1, total, ROWS, WIDE), F32),
            pltpu.VMEM((turned, 2, 2, ROWS, HALF), F32),
            pltpu.VMEM((HALF, 2 * WIDE), F32),
            pltpu.VMEM((ROWS, PMAX), F32),
            pltpu.VMEM((PMAX, 2 * PMAX), F32),
            dma,
            dma((36,)),
            dma((36,)),
            dma((8 * total,)),
            dma((8 * total,)),
            dma((4 * turned,)),
            dma((4 * turned,)),
            dma((SIDE - 1,)),
            dma((SIDE - 1,)),
            dma((CHIPS - 1,)),
            dma((CHIPS - 1,)),
            dma,
        ],
        compiler_params=pltpu.CompilerParams(collective_id=1, has_side_effects=True),
        cost_estimate=pl.CostEstimate(flops=400_000_000, bytes_accessed=25_000_000, transcendentals=0),
        name="post",
    )(weights, pivots, places, columns, inverse, moved, later, front)


def parent_kernel(
    order_ref, pivots_ref, own_ref, here_ref, inverse_ref, sum_ref, mirror_ref, front_ref, panel_ref, schur_ref, weights
):
    step = pl.program_id(0)
    grid_rank = lax.axis_index("grid")
    sums = len(TURNED) + len(SELF)

    @pl.when(step == 0)
    def _():
        inverse = inverse_ref[...]
        panel = exact(own_ref[...], inverse, NT)
        panel_ref[...] = panel
        weights[...] = exact(panel, inverse, NN)

    total = front_ref[...] - product(here_ref[...], weights[...], NT).T
    pivots = pivots_ref[0]
    rows = grid_rank * ROWS + lax.broadcasted_iota(jnp.int32, (ROWS, WIDE), 0)
    columns = order_ref[step] * WIDE + lax.broadcasted_iota(jnp.int32, (ROWS, WIDE), 1)
    keep = (rows >= pivots) & (columns >= pivots)

    @pl.when(step < sums)
    def _():
        schur_ref[...] = jnp.where(keep, total + sum_ref[0], 0.0)

    @pl.when(step >= sums)
    def _():
        mirror = jnp.concatenate([mirror_ref[0, k, half] for k in range(2) for half in range(2)], axis=1)
        schur_ref[...] = jnp.where(keep, total + mirror, 0.0)


def parent_schur(order, pivots, columns, inverse, sums, mirror, front):
    count = len(TURNED) + len(SELF)
    spec = pltpu.PrefetchScalarGridSpec(
        num_scalar_prefetch=1,
        grid=(CHIPS,),
        in_specs=[
            pl.BlockSpec(memory_space=pltpu.SMEM),
            pl.BlockSpec((ROWS, PMAX), lambda i, order: (order[CHIPS], 0)),
            pl.BlockSpec((WIDE, PMAX), lambda i, order: (order[i], 0)),
            pl.BlockSpec((PMAX, PMAX), lambda i, order: (0, 0)),
            pl.BlockSpec((1, ROWS, WIDE), lambda i, order: (jnp.minimum(i, count - 1), 0, 0)),
            pl.BlockSpec((1, 2, 2, ROWS, HALF), lambda i, order: (jnp.maximum(i - count, 0), 0, 0, 0, 0)),
            pl.BlockSpec((ROWS, WIDE), lambda i, order: (0, order[i])),
        ],
        out_specs=(
            pl.BlockSpec((ROWS, PMAX), lambda i, order: (0, 0)),
            pl.BlockSpec((ROWS, WIDE), lambda i, order: (0, order[i])),
        ),
        scratch_shapes=[pltpu.VMEM((ROWS, PMAX), F32)],
    )
    return pl.pallas_call(
        parent_kernel,
        grid_spec=spec,
        out_shape=(jax.ShapeDtypeStruct((ROWS, PMAX), F32), jax.ShapeDtypeStruct((ROWS, ORDER), F32)),
        cost_estimate=pl.CostEstimate(flops=400_000_000, bytes_accessed=30_000_000, transcendentals=0),
        name="parent_schur",
    )(order, pivots, columns, columns, inverse, sums, mirror, front)


def on_device(child_fronts, parent_fronts, child_maps, parent_of, child_pivots, parent_pivots):
    front_group = lax.axis_index("front")
    rank = lax.axis_index("grid")
    chip = rank // 2
    front_rows = child_fronts[0]
    pivots = lax.dynamic_slice(child_pivots, (front_group,), (1,))
    upper_pivots = lax.dynamic_slice(parent_pivots, (front_group,), (1,))
    groups = (front_group - jnp.arange(SIDE, dtype=jnp.int32)) % SIDE
    weights = (parent_of[groups] == front_group).astype(F32)
    number = jnp.arange(CHIPS + 1, dtype=jnp.int32)
    count = len(TURNED) + len(SELF)
    sign = jnp.where(number < count, 1, -1)
    order = offset_chip(chip, jnp.where(number < count, number, number - count), sign)
    order = jnp.where(number < CHIPS, order, rank)

    position = jnp.arange(ORDER, dtype=jnp.int32)
    line = jnp.where(position >= pivots, child_maps[front_group], -1)
    line = jnp.pad(line, (0, 2 * WIDE), constant_values=-1)
    places = jnp.broadcast_to(line[None], (8, line.shape[0]))
    columns, turned, later = front(front_rows, places)
    same_core = [[2 * c + k for c in range(CHIPS)] for k in range(2)]
    moved = lax.all_to_all(turned, "grid", 0, 0, axis_index_groups=same_core)
    inverse = inverse_factor(pivots, columns)
    panel_rows, upper_columns, upper_inverse, sums, mirror = post(
        weights, upper_pivots, places, columns, inverse, moved, later, parent_fronts[0]
    )
    upper_panel, upper_schur = parent_schur(
        order, upper_pivots, upper_columns, upper_inverse, sums, mirror, parent_fronts[0]
    )
    return (panel_rows[None], upper_panel[None], upper_schur[None])


def solution(mesh):
    in_specs = (P("front", "grid", None), P("front", "grid", None), P(), P(), P(), P())
    out_specs = (P("front", "grid", None), P("front", "grid", None), P("front", "grid", None))
    return jax.shard_map(
        on_device, mesh=mesh, in_specs=in_specs, out_specs=out_specs, check_vma=False
    )
```
